32 devices in a mesh: ta: 4 (over y, x), gy: 2 (over core), gx: 4 (over z).
Axes of the slice: x: 2, y: 2, z: 4, core: 2. Of those that a mesh axis runs over, the one named last changes fastest.
Arguments:
- features: bfloat16 [16, 4, 416, 192], P('ta', 'gy', 'gx'), may hold values from -6 to 6
- gain_first: float32 [192], replicated, may hold values from 0.1 to 1.9
- kernel_first: bfloat16 [3, 3, 3, 192, 192], replicated, may hold values from -0.078125 to 0.078125
- bias_first: float32 [192], replicated, may hold values from -3 to 3
- gain_second: float32 [192], replicated, may hold values from 0.1 to 1.9
- kernel_second: bfloat16 [3, 3, 3, 192, 192], replicated, may hold values from -0.078125 to 0.078125
- bias_second: float32 [192], replicated, may hold values from -3 to 3
Outputs:
- block_out: bfloat16 [16, 4, 416, 192], P('ta', 'gy', 'gx')
The draws below stay inside these ranges and needn't reach their ends.
All inputs are finite; a program needn't handle non-finite values.
Results may differ from the reference program's by a relative error of at most 0.0075.
Values may be sent and summed in bfloat16 or wider, within the bound.
A program may use at most 64 MiB of HBM per device.

```python
import jax
import jax.numpy as jnp
from jax import lax

C = 192
W = 416
FRAMES = 16
H = 4


def levels(stream_key, dims, split, low, top_value):
    level = 1.0
    for dim, parts in split:
        heights = jax.random.uniform(jax.random.fold_in(jax.random.fold_in(stream_key, 6), dim), (parts,), jnp.float32, low / len(split), top_value / len(split))
        level = level * jnp.repeat(jnp.exp(heights), dims[dim] // parts).reshape((-1,) + (1,) * (len(dims) - 1 - dim))
    return level


def bell_draw(stream_key, dims, spread, bound, cuts=(), kind=jnp.bfloat16):
    factor_of = levels(stream_key, dims, cuts, -0.22, 0.18) if cuts else 1.0
    array = jax.random.normal(stream_key, dims, jnp.float32) * spread * factor_of
    return jnp.minimum(jnp.maximum(array, -bound), bound).astype(kind)


def setup_inputs(seed: int = 0) -> dict:
    streams_of = jax.random.split(jax.random.key(seed), 8)
    features = bell_draw(streams_of[0], (FRAMES, H, W, C), 1.0, 6.0, ((0, 4), (1, 2), (2, 4)))
    gain_first = jnp.clip(1.0 + 0.18 * jax.random.normal(streams_of[1], (C,), jnp.float32), 0.1, 1.9)
    kernel_first = bell_draw(streams_of[2], (3, 3, 3, C, C), (27 * C) ** -0.5, 0.078125)
    bias_first = bell_draw(streams_of[3], (C,), 0.5, 3.0, (), jnp.float32)
    gain_second = jnp.clip(1.0 + 0.18 * jax.random.normal(streams_of[4], (C,), jnp.float32), 0.1, 1.9)
    kernel_second = bell_draw(streams_of[5], (3, 3, 3, C, C), (27 * C) ** -0.5, 0.078125)
    bias_second = bell_draw(streams_of[6], (C,), 0.5, 3.0, (), jnp.float32)
    return dict(features=features, gain_first=gain_first, kernel_first=kernel_first, bias_first=bias_first, gain_second=gain_second, kernel_second=kernel_second, bias_second=bias_second)


epsilon = 1e-06

def activate(field, gain):
    field = field.astype(jnp.float32)
    meansq = lax.optimization_barrier(jnp.mean(field * field, axis=-1, keepdims=True))
    return jax.nn.silu(field * lax.rsqrt(meansq + epsilon) * gain).astype(jnp.bfloat16)

def convolve(source, kernel, bias):
    frames, rows, cols, channels = source.shape
    padded = jnp.pad(source, ((2, 0), (1, 1), (1, 1), (0, 0)))

    def one_frame(index):
        window = lax.dynamic_slice_in_dim(padded, index, 3, 0)
        total = jnp.zeros((rows * cols, kernel.shape[-1]), jnp.float32)
        for delta_t in range(3):
            for delta_y in range(3):
                for delta_x in range(3):
                    piece = window[delta_t, delta_y:delta_y + rows, delta_x:delta_x + cols].reshape(-1, channels)
                    total = total + jnp.dot(piece, kernel[delta_t, delta_y, delta_x], preferred_element_type=jnp.float32)
        return total.reshape(rows, cols, -1) + bias
    return lax.map(one_frame, jnp.arange(frames, dtype=jnp.int32))

def reference(features, gain_first, kernel_first, bias_first, gain_second, kernel_second, bias_second):
    first = activate(features, gain_first)
    middle = convolve(first, kernel_first, bias_first).astype(jnp.bfloat16)
    second = activate(middle, gain_second)
    result = convolve(second, kernel_second, bias_second) + features.astype(jnp.float32)
    return result.astype(jnp.bfloat16)
```

```python
import jax
import jax.numpy as jnp
from jax import lax
from jax.experimental import pallas as pl
from jax.experimental.pallas import tpu as pltpu
from jax.sharding import PartitionSpec as P

epsilon = 1e-06
AXES = ("ta", "gy", "gx")
NOW, PAST = 0, 1
PACK = 16
MATMUL = 256


def activate(field, gain):
    meansq = jnp.mean(field * field, axis=0, keepdims=True)
    u = field * lax.rsqrt(meansq + epsilon) * gain
    return u / (1.0 + jnp.exp(-u))


def message_numbers(frames, rows):
    names = [("edge", kind, dy, dx) for kind in (NOW, PAST) for dy in (-1, 0, 1) for dx in (-1, 1)]
    names += [("rows1", side) for side in range(2)]
    names += [("rows2", f, side) for f in range(frames) for side in range(2)]
    names += [("past1", o) for o in range(rows)]
    names += [("past2", i, o) for i in range(2) for o in range(rows)]
    names += [("pass1", side) for side in range(2)]
    names += [("pass2", i, side) for i in range(2) for side in range(2)]
    return {name: n for n, name in enumerate(names)}


def block_kernel(
    feat, gain1, bias1, gain2, bias2, k1, k2, out,
    fin, fout, raw, wt, vec_raw, vec, plane, past, rows_in, edge_out, edge_in, halo, x, zero, acc,
    vec_sem, in_sem, w_sem, out_sem, send_sem, recv_sem,
):
    frames, rows, ch, cols = fin.shape
    lanes = plane.shape[-1]
    bf16, f32 = jnp.bfloat16, jnp.float32
    taps = 9 * ch
    padded = wt.shape[-1]
    groups = ch // PACK
    width = 2 * frames * rows
    per = lanes // width
    number = message_numbers(frames, rows)
    me = {a: lax.axis_index(a) for a in AXES}
    size = {a: lax.axis_size(a) for a in AXES}
    ta, gy, gx = (me[a] for a in AXES)

    def at(dt, dy, dx):
        place = {"ta": ta + dt, "gy": gy + dy, "gx": gx + dx}
        ok = None
        for a, d in zip(AXES, (dt, dy, dx)):
            if isinstance(d, int) and d == 0:
                continue
            inside = (place[a] >= 0) & (place[a] < size[a])
            ok = inside if ok is None else ok & inside
        return ok, place

    moves = [(0, dy, dx) for dy in (-1, 0, 1) for dx in (-1, 0, 1) if dy or dx]
    moves += [(1, 0, 0)] + [(1, dy, dx) for dy in (-1, 0, 1) for dx in (-1, 1)]
    barrier = pltpu.get_barrier_semaphore()
    expected = jnp.int32(0)
    for dt, dy, dx in moves:
        ok, source = at(-dt, -dy, -dx)

        @pl.when(ok)
        def _():
            pl.semaphore_signal(
                barrier, inc=1, device_id=source, device_id_type=pl.DeviceIdType.MESH
            )

        expected = expected + at(dt, dy, dx)[0].astype(jnp.int32)

    fin_copies = [pltpu.make_async_copy(feat.at[f], fin.at[f], in_sem.at[f]) for f in range(frames)]
    for f in reversed(range(frames)):
        fin_copies[f].start()
    vec_copies = [
        pltpu.make_async_copy(v, vec_raw.at[i], vec_sem.at[i])
        for i, v in enumerate((gain1, bias1, gain2, bias2))
    ]
    for copy in vec_copies:
        copy.start()
    w_copies = [
        [
            pltpu.make_async_copy(
                k.at[pl.ds(p * taps, taps)], raw.at[layer, pl.ds(p * taps, taps)], w_sem.at[layer, p]
            )
            for p in range(3)
        ]
        for layer, k in enumerate((k1, k2))
    ]
    for layer in range(2):
        for p in (2, 1, 0):
            w_copies[layer][p].start()

    def copy_to(name, src, dst, target):
        n = number[name] if isinstance(name, tuple) else name
        return pltpu.make_async_remote_copy(
            src_ref=src,
            dst_ref=dst,
            send_sem=send_sem.at[n],
            recv_sem=recv_sem.at[n],
            device_id=target,
            device_id_type=pl.DeviceIdType.MESH,
        )

    def edge_copy(kind, dy, dx):
        side = (dx + 1) // 2
        target = at(kind, dy, dx)[1]
        return copy_to(("edge", kind, dy, dx), edge_out.at[side], edge_in.at[kind, dy + 1, side], target)

    def line(dy):
        return rows - 1 if dy > 0 else 0

    def rows1_copy(side):
        dy = 1 if side == 0 else -1
        src = plane.at[0, :, line(dy)]
        return copy_to(("rows1", side), src, rows_in.at[0, side, pl.ds(2, frames)], at(0, dy, 0)[1])

    def rows2_copy(f, side):
        dy = 1 if side == 0 else -1
        src = plane.at[1, f, line(dy)]
        return copy_to(("rows2", f, side), src, rows_in.at[1, side, 2 + f], at(0, dy, 0)[1])

    def turn(o):
        return jnp.where(gy == 0, rows - 1 - o, o)

    def past1_copy(o):
        r = turn(o)
        src = plane.at[0, pl.ds(frames - 2, 2), r]
        return copy_to(("past1", o), src, past.at[0, :, r], at(1, 0, 0)[1])

    def past2_copy(i, o):
        r = turn(o)
        return copy_to(("past2", i, o), plane.at[1, frames - 2 + i, r], past.at[1, i, r], at(1, 0, 0)[1])

    def pass1_copy(side):
        dy = 1 if side == 0 else -1
        dst = rows_in.at[0, side, pl.ds(0, 2)]
        return copy_to(("pass1", side), past.at[0, :, line(dy)], dst, at(0, dy, 0)[1])

    def pass2_copy(i, side):
        dy = 1 if side == 0 else -1
        dst = rows_in.at[1, side, i]
        return copy_to(("pass2", i, side), past.at[1, i, line(dy)], dst, at(0, dy, 0)[1])

    has_past, has_next = ta > 0, ta < size["ta"] - 1
    from_side = (gy > 0, gy < size["gy"] - 1)
    to_side = (gy < size["gy"] - 1, gy > 0)

    for side in range(2):
        @pl.when(jnp.logical_not(from_side[side]))
        def _():
            rows_in[:, side] = jnp.zeros((2, frames + 2, ch, lanes), bf16)

    @pl.when(jnp.logical_not(has_past))
    def _():
        past[...] = jnp.zeros_like(past)
        rows_in[:, :, 0:2] = jnp.zeros((2, 2, 2, ch, lanes), bf16)

    for kind in (NOW, PAST):
        for dy in (-1, 0, 1):
            for dx in (-1, 1):
                @pl.when(jnp.logical_not(at(-kind, -dy, -dx)[0]))
                def _():
                    edge_in[kind, dy + 1, (dx + 1) // 2] = jnp.zeros(edge_in.shape[3:], bf16)

    plane[0] = jnp.zeros(plane.shape[1:], bf16)
    zero[...] = jnp.zeros_like(zero)
    if padded > taps:
        for layer in range(2):
            for p in range(3):
                wt[layer, p, :, taps:padded] = jnp.zeros((ch, padded - taps), bf16)
    for i, copy in enumerate(vec_copies):
        copy.wait()
        vec[i] = jnp.broadcast_to(vec_raw[i], (lanes, ch)).T

    lane = lax.broadcasted_iota(jnp.int32, (1, lanes), 1)

    for f in reversed(range(frames)):
        fin_copies[f].wait()
        for row in range(rows):
            value = activate(fin[f, row].astype(f32), vec[0, :, 0:cols])
            plane[0, f, row, :, 0:cols] = value.astype(bf16)

    def place(v, shift):
        shift = shift % lanes
        return pltpu.roll(v, shift, 1) if shift else v

    lane_pack = lax.broadcasted_iota(jnp.int32, (PACK, lanes), 1)

    def within(low, count):
        return (lane_pack >= low) & (lane_pack < low + count)

    for side in range(2):
        first_col = 0 if side == 0 else cols - 2
        for b in range(edge_out.shape[1] // PACK):
            total = jnp.zeros((PACK, lanes), bf16)
            for f in range(frames):
                for row in range(rows):
                    slot = 2 * (f * rows + row)
                    for g in range(b * per, min(groups, (b + 1) * per)):
                        low = (g - b * per) * width + slot
                        v = plane[0, f, row, g * PACK : (g + 1) * PACK, :]
                        total = jnp.where(within(low, 2), place(v, low - first_col), total)
            edge_out[side, b * PACK : (b + 1) * PACK, :] = total

    pl.semaphore_wait(barrier, expected)
    for dy in (0, -1, 1):
        for dx in (-1, 1):
            pl.when(at(0, dy, dx)[0])(edge_copy(NOW, dy, dx).start)
    for side in range(2):
        pl.when(to_side[side])(rows1_copy(side).start)

    @pl.when(has_next)
    def _():
        for o in range(rows):
            past1_copy(o).start()

    for dy in (0, -1, 1):
        for dx in (-1, 1):
            pl.when(at(1, dy, dx)[0])(edge_copy(PAST, dy, dx).start)

    def transpose_weights(layer):
        for p in (2, 1, 0):
            w_copies[layer][p].wait()
            for low in range(0, taps, lanes):
                count = min(lanes, taps - low)
                block = raw[layer, p * taps + low : p * taps + low + count, :]
                wt[layer, p, :, low : low + count] = block.T

    transpose_weights(0)
    transpose_weights(1)

    def receive_edges(kind):
        for dy in (-1, 0, 1):
            for dx in (-1, 1):
                pl.when(at(-kind, -dy, -dx)[0])(edge_copy(kind, dy, dx).wait_recv)
        apart = lanes - 2 - cols
        for dy in (-1, 0, 1):
            for g in range(groups):
                b, low = g // per, (g % per) * width
                right = edge_in[kind, dy + 1, 0, b * PACK : (b + 1) * PACK, :]
                left = edge_in[kind, dy + 1, 1, b * PACK : (b + 1) * PACK, :]
                both = jnp.where(within(0, width), place(right, -low), place(left, apart - low))
                halo[kind, dy + 1, g * PACK : (g + 1) * PACK, :] = both

    lane_ch = lax.broadcasted_iota(jnp.int32, (ch, lanes), 1)
    at_halo = ((lane_ch >= cols) & (lane_ch < cols + 2)) | (lane_ch >= lanes - 2)

    def spread(layer, slot):
        for j in range(rows + 2):
            side = 0 if j == 0 else 1
            if j in (0, rows + 1):
                v = rows_in[layer, side, slot]
            elif slot < 2:
                v = past[layer, slot, j - 1]
            else:
                v = plane[layer, slot - 2, j - 1]
            if layer == 0:
                kind = PAST if slot < 2 else NOW
                dy = 1 if j == 0 else -1 if j == rows + 1 else 0
                f = slot + frames - 2 if slot < 2 else slot - 2
                index = 2 * (f * rows + (line(dy) if dy else j - 1))
                v = jnp.where(at_halo, place(halo[kind, dy + 1], cols - index), v)
            low = j * lanes
            x[layer, slot, 0:ch, low : low + lanes] = place(v, 1)
            x[layer, slot, ch : 2 * ch, low : low + lanes] = v
            x[layer, slot, 2 * ch : 3 * ch, low : low + lanes] = place(v, -1)

    def conv(layer, terms):
        left, right = [], []
        for slot, p in terms:
            left.append(wt[layer, p])
            right += [x[layer, slot, :, q * lanes : (q + rows) * lanes] for q in range(3)]
            if padded > taps:
                right.append(zero[...])
        lhs = left[0] if len(left) == 1 else jnp.concatenate(left, axis=1)
        rhs = jnp.concatenate(right, axis=0)
        return jnp.dot(lhs, rhs, preferred_element_type=f32)

    keep = (lane < cols) | ((lane == cols) & (gx < size["gx"] - 1)) | ((lane == lanes - 1) & (gx > 0))

    def middle(f, total):
        for row in range(rows):
            value = total[:, row * lanes : (row + 1) * lanes] + vec[1]
            value = activate(value.astype(bf16).astype(f32), vec[2])
            plane[1, f, row] = jnp.where(keep, value, 0.0).astype(bf16)
        for side in range(2):
            pl.when(to_side[side])(rows2_copy(f, side).start)
        if f >= frames - 2:
            @pl.when(has_next)
            def _():
                for o in range(rows):
                    past2_copy(f - frames + 2, o).start()

    def finish(f, total):
        for row in range(rows):
            value = total[:, row * lanes : row * lanes + cols] + vec[3, :, 0:cols]
            fout[f, row] = (value + fin[f, row].astype(f32)).astype(bf16)
        pltpu.make_async_copy(fout.at[f], out.at[f], out_sem.at[f]).start()

    for side in range(2):
        pl.when(from_side[side])(rows1_copy(side).wait_recv)
    receive_edges(NOW)
    for slot in range(2, frames + 2):
        spread(0, slot)
    for f in range(2, frames):
        middle(f, conv(0, [(f + p, p) for p in range(3)]))

    @pl.when(has_past)
    def _():
        past1_copy(0).wait_recv()
        for side in range(2):
            pl.when(to_side[side] & (turn(0) == line(1 - 2 * side)))(pass1_copy(side).start)
        for o in range(1, rows):
            past1_copy(o).wait_recv()
        for side in range(2):
            pl.when(to_side[side] & (turn(0) != line(1 - 2 * side)))(pass1_copy(side).start)

    acc[0] = conv(0, [(2, 2)])
    acc[1] = conv(0, [(2, 1), (3, 2)])
    for side in range(2):
        pl.when(has_past & from_side[side])(pass1_copy(side).wait_recv)
    receive_edges(PAST)
    for slot in range(2):
        spread(0, slot)
    middle(1, acc[1] + conv(0, [(1, 0)]))
    middle(0, acc[0] + conv(0, [(0, 0), (1, 1)]))

    def receive_rows2(f):
        for side in range(2):
            pl.when(from_side[side])(rows2_copy(f, side).wait_recv)
        spread(1, f + 2)

    for f in range(2, frames):
        receive_rows2(f)
    acc[2] = conv(1, [(4, 2)])
    acc[3] = conv(1, [(4, 1), (5, 2)])

    def pass_on(i):
        @pl.when(has_past)
        def _():
            past2_copy(i, 0).wait_recv()
            for side in range(2):
                pl.when(to_side[side] & (turn(0) == line(1 - 2 * side)))(pass2_copy(i, side).start)
            for o in range(1, rows):
                past2_copy(i, o).wait_recv()
            for side in range(2):
                pl.when(to_side[side] & (turn(0) != line(1 - 2 * side)))(pass2_copy(i, side).start)

    for f in (1, 0):
        receive_rows2(f)
    finish(3, acc[3] + conv(1, [(3, 0)]))
    finish(2, acc[2] + conv(1, [(2, 0), (3, 1)]))
    pass_on(0)
    acc[1] = conv(1, [(2, 1), (3, 2)])
    pass_on(1)
    acc[0] = conv(1, [(2, 2)])
    for i in range(2):
        for side in range(2):
            pl.when(has_past & from_side[side])(pass2_copy(i, side).wait_recv)
        spread(1, i)
    finish(1, acc[1] + conv(1, [(1, 0)]))
    finish(0, acc[0] + conv(1, [(0, 0), (1, 1)]))

    for kind in (NOW, PAST):
        for dy in (-1, 0, 1):
            for dx in (-1, 1):
                pl.when(at(kind, dy, dx)[0])(edge_copy(kind, dy, dx).wait_send)
    for side in range(2):
        @pl.when(to_side[side])
        def _():
            rows1_copy(side).wait_send()
            for f in range(frames):
                rows2_copy(f, side).wait_send()

        @pl.when(to_side[side] & has_past)
        def _():
            pass1_copy(side).wait_send()
            for i in range(2):
                pass2_copy(i, side).wait_send()

    @pl.when(has_next)
    def _():
        for o in range(rows):
            past1_copy(o).wait_send()
            for i in range(2):
                past2_copy(i, o).wait_send()

    for f in range(frames):
        pltpu.make_async_copy(fout.at[f], out.at[f], out_sem.at[f]).wait()


def local(features, gain_first, kernel_first, bias_first, gain_second, kernel_second, bias_second):
    frames, rows, cols, ch = features.shape
    lanes = -(-(cols + 4) // 128) * 128
    padded = -(-9 * ch // MATMUL) * MATMUL
    per = lanes // (2 * frames * rows)
    blocks = -(-(ch // PACK) // per)
    hbm = pl.BlockSpec(memory_space=pl.ANY)
    bf16, f32 = jnp.bfloat16, jnp.float32
    messages = len(message_numbers(frames, rows))
    dma = pltpu.SemaphoreType.DMA
    result = pl.pallas_call(
        block_kernel,
        out_shape=jax.ShapeDtypeStruct((frames, rows, ch, cols), bf16),
        in_specs=[hbm] * 7,
        out_specs=hbm,
        scratch_shapes=[
            pltpu.VMEM((frames, rows, ch, cols), bf16),
            pltpu.VMEM((frames, rows, ch, cols), bf16),
            pltpu.VMEM((2, 27 * ch, ch), bf16),
            pltpu.VMEM((2, 3, ch, padded), bf16),
            pltpu.VMEM((4, 1, ch), f32),
            pltpu.VMEM((4, ch, lanes), f32),
            pltpu.VMEM((2, frames, rows, ch, lanes), bf16),
            pltpu.VMEM((2, 2, rows, ch, lanes), bf16),
            pltpu.VMEM((2, 2, frames + 2, ch, lanes), bf16),
            pltpu.VMEM((2, blocks * PACK, lanes), bf16),
            pltpu.VMEM((2, 3, 2, blocks * PACK, lanes), bf16),
            pltpu.VMEM((2, 3, ch, lanes), bf16),
            pltpu.VMEM((2, frames + 2, 3 * ch, (rows + 2) * lanes), bf16),
            pltpu.VMEM((max(padded - 9 * ch, PACK), rows * lanes), bf16),
            pltpu.VMEM((frames, ch, rows * lanes), f32),
            dma((4,)),
            dma((frames,)),
            dma((2, 3)),
            dma((frames,)),
            dma((messages,)),
            dma((messages,)),
        ],
        compiler_params=pltpu.CompilerParams(
            collective_id=0, has_side_effects=True, vmem_limit_bytes=56 * 1024 * 1024
        ),
        name="residual_block",
    )(
        jnp.swapaxes(features, 2, 3),
        gain_first.reshape(1, ch),
        bias_first.reshape(1, ch),
        gain_second.reshape(1, ch),
        bias_second.reshape(1, ch),
        kernel_first.reshape(27 * ch, ch),
        kernel_second.reshape(27 * ch, ch),
    )
    return jnp.swapaxes(result, 2, 3)


def solution(mesh):
    placed = (P("ta", "gy", "gx", None), P(), P(), P(), P(), P(), P())
    return jax.shard_map(
        local, mesh=mesh, in_specs=placed, out_specs=P("ta", "gy", "gx", None), check_vma=False
    )
```

```python
import jax
import jax.numpy as jnp
from jax import lax
from jax.experimental import pallas as pl
from jax.experimental.pallas import tpu as pltpu
from jax.sharding import PartitionSpec as P

epsilon = 1e-06
AXES = ("ta", "gy", "gx")
NOW, PAST = 0, 1
PACK = 16
MATMUL = 256


def activate(field, gain):
    meansq = jnp.mean(field * field, axis=0, keepdims=True)
    u = field * lax.rsqrt(meansq + epsilon) * gain
    return u / (1.0 + jnp.exp(-u))


def message_numbers(frames, rows):
    names = [("edge", kind, dy, dx) for kind in (NOW, PAST) for dy in (-1, 0, 1) for dx in (-1, 1)]
    names += [("rows1", side) for side in range(2)]
    names += [("rows2", f, side) for f in range(frames) for side in range(2)]
    names += [("past1", o) for o in range(rows)]
    names += [("past2", i, o) for i in range(2) for o in range(rows)]
    names += [("pass1", side) for side in range(2)]
    names += [("pass2", i, side) for i in range(2) for side in range(2)]
    return {name: n for n, name in enumerate(names)}


def block_kernel(
    feat, gain1, bias1, gain2, bias2, k1, k2, out,
    fin, raw, wt, vec_raw, vec, plane, past, rows_in, edge_out, edge_in, halo, x, zero, acc,
    vec_sem, in_sem, w_sem, send_sem, recv_sem,
):
    frames, rows, ch, cols = fin.shape
    lanes = plane.shape[-1]
    bf16, f32 = jnp.bfloat16, jnp.float32
    taps = 9 * ch
    padded = wt.shape[2] * lanes
    groups = ch // PACK
    width = 2 * frames * rows
    per = lanes // width
    number = message_numbers(frames, rows)
    me = {a: lax.axis_index(a) for a in AXES}
    size = {a: lax.axis_size(a) for a in AXES}
    ta, gy, gx = (me[a] for a in AXES)

    def at(dt, dy, dx):
        place = {"ta": ta + dt, "gy": gy + dy, "gx": gx + dx}
        ok = None
        for a, d in zip(AXES, (dt, dy, dx)):
            if isinstance(d, int) and d == 0:
                continue
            inside = (place[a] >= 0) & (place[a] < size[a])
            ok = inside if ok is None else ok & inside
        return ok, place

    moves = [(0, dy, dx) for dy in (-1, 0, 1) for dx in (-1, 0, 1) if dy or dx]
    moves += [(1, 0, 0)] + [(1, dy, dx) for dy in (-1, 0, 1) for dx in (-1, 1)]
    barrier = pltpu.get_barrier_semaphore()
    expected = jnp.int32(0)
    for dt, dy, dx in moves:
        ok, source = at(-dt, -dy, -dx)

        @pl.when(ok)
        def _():
            pl.semaphore_signal(
                barrier, inc=1, device_id=source, device_id_type=pl.DeviceIdType.MESH
            )

        expected = expected + at(dt, dy, dx)[0].astype(jnp.int32)

    fin_copies = [pltpu.make_async_copy(feat.at[f], fin.at[f], in_sem.at[f]) for f in range(frames)]
    for f in reversed(range(frames)):
        fin_copies[f].start()
    vec_copies = [
        pltpu.make_async_copy(v, vec_raw.at[i], vec_sem.at[i])
        for i, v in enumerate((gain1, bias1, gain2, bias2))
    ]
    for copy in vec_copies:
        copy.start()
    w_copies = [
        [
            pltpu.make_async_copy(
                k.at[pl.ds(p * taps, taps)], raw.at[layer, pl.ds(p * taps, taps)], w_sem.at[layer, p]
            )
            for p in range(3)
        ]
        for layer, k in enumerate((k1, k2))
    ]
    for layer in range(2):
        for p in (2, 1, 0):
            w_copies[layer][p].start()

    def copy_to(name, src, dst, target):
        n = number[name] if isinstance(name, tuple) else name
        return pltpu.make_async_remote_copy(
            src_ref=src,
            dst_ref=dst,
            send_sem=send_sem.at[n],
            recv_sem=recv_sem.at[n],
            device_id=target,
            device_id_type=pl.DeviceIdType.MESH,
        )

    def edge_copy(kind, dy, dx):
        side = (dx + 1) // 2
        target = at(kind, dy, dx)[1]
        return copy_to(("edge", kind, dy, dx), edge_out.at[side], edge_in.at[kind, dy + 1, side], target)

    def line(dy):
        return rows - 1 if dy > 0 else 0

    def rows1_copy(side):
        dy = 1 if side == 0 else -1
        src = plane.at[0, :, line(dy)]
        return copy_to(("rows1", side), src, rows_in.at[0, side, pl.ds(2, frames)], at(0, dy, 0)[1])

    def rows2_copy(f, side):
        dy = 1 if side == 0 else -1
        src = plane.at[1, f, line(dy)]
        return copy_to(("rows2", f, side), src, rows_in.at[1, side, 2 + f], at(0, dy, 0)[1])

    def turn(o):
        return jnp.where(gy == 0, rows - 1 - o, o)

    def past1_copy(o):
        r = turn(o)
        src = plane.at[0, pl.ds(frames - 2, 2), r]
        return copy_to(("past1", o), src, past.at[0, :, r], at(1, 0, 0)[1])

    def past2_copy(i, o):
        r = turn(o)
        return copy_to(("past2", i, o), plane.at[1, frames - 2 + i, r], past.at[1, i, r], at(1, 0, 0)[1])

    def pass1_copy(side):
        dy = 1 if side == 0 else -1
        dst = rows_in.at[0, side, pl.ds(0, 2)]
        return copy_to(("pass1", side), past.at[0, :, line(dy)], dst, at(0, dy, 0)[1])

    def pass2_copy(i, side):
        dy = 1 if side == 0 else -1
        dst = rows_in.at[1, side, i]
        return copy_to(("pass2", i, side), past.at[1, i, line(dy)], dst, at(0, dy, 0)[1])

    has_past, has_next = ta > 0, ta < size["ta"] - 1
    from_side = (gy > 0, gy < size["gy"] - 1)
    to_side = (gy < size["gy"] - 1, gy > 0)

    for side in range(2):
        @pl.when(jnp.logical_not(from_side[side]))
        def _():
            rows_in[:, side] = jnp.zeros((2, frames + 2, ch, lanes), bf16)

    @pl.when(jnp.logical_not(has_past))
    def _():
        past[...] = jnp.zeros_like(past)
        rows_in[:, :, 0:2] = jnp.zeros((2, 2, 2, ch, lanes), bf16)

    for kind in (NOW, PAST):
        for dy in (-1, 0, 1):
            for dx in (-1, 1):
                @pl.when(jnp.logical_not(at(-kind, -dy, -dx)[0]))
                def _():
                    edge_in[kind, dy + 1, (dx + 1) // 2] = jnp.zeros(edge_in.shape[3:], bf16)

    plane[0] = jnp.zeros(plane.shape[1:], bf16)
    zero[...] = jnp.zeros_like(zero)
    if padded > taps:
        for layer in range(2):
            for p in range(3):
                for low in range(taps // lanes * lanes, padded, lanes):
                    wt[layer, p, low // lanes] = jnp.zeros((ch, lanes), bf16)
    for i, copy in enumerate(vec_copies):
        copy.wait()
        vec[i] = jnp.broadcast_to(vec_raw[i], (lanes, ch)).T

    lane = lax.broadcasted_iota(jnp.int32, (1, lanes), 1)

    for f in reversed(range(frames)):
        fin_copies[f].wait()
        for row in range(rows):
            value = activate(fin[f, row].astype(f32), vec[0, :, 0:cols])
            plane[0, f, row, :, 0:cols] = value.astype(bf16)

    def place(v, shift):
        shift = shift % lanes
        return pltpu.roll(v, shift, 1) if shift else v

    lane_pack = lax.broadcasted_iota(jnp.int32, (PACK, lanes), 1)

    def within(low, count):
        return (lane_pack >= low) & (lane_pack < low + count)

    for side in range(2):
        first_col = 0 if side == 0 else cols - 2
        for b in range(edge_out.shape[1] // PACK):
            total = jnp.zeros((PACK, lanes), bf16)
            for f in range(frames):
                for row in range(rows):
                    slot = 2 * (f * rows + row)
                    for g in range(b * per, min(groups, (b + 1) * per)):
                        low = (g - b * per) * width + slot
                        v = plane[0, f, row, g * PACK : (g + 1) * PACK, :]
                        total = jnp.where(within(low, 2), place(v, low - first_col), total)
            edge_out[side, b * PACK : (b + 1) * PACK, :] = total

    pl.semaphore_wait(barrier, expected)
    for dy in (0, -1, 1):
        for dx in (-1, 1):
            pl.when(at(0, dy, dx)[0])(edge_copy(NOW, dy, dx).start)
    for side in range(2):
        pl.when(to_side[side])(rows1_copy(side).start)

    @pl.when(has_next)
    def _():
        for o in range(rows):
            past1_copy(o).start()

    for dy in (0, -1, 1):
        for dx in (-1, 1):
            pl.when(at(1, dy, dx)[0])(edge_copy(PAST, dy, dx).start)

    def transpose_weights(layer):
        for p in (2, 1, 0):
            w_copies[layer][p].wait()
            for low in range(0, taps, lanes):
                count = min(lanes, taps - low)
                block = raw[layer, p * taps + low : p * taps + low + count, :]
                wt[layer, p, low // lanes, :, 0:count] = block.T

    transpose_weights(0)
    transpose_weights(1)

    def receive_edges(kind):
        for dy in (-1, 0, 1):
            for dx in (-1, 1):
                pl.when(at(-kind, -dy, -dx)[0])(edge_copy(kind, dy, dx).wait_recv)
        apart = lanes - 2 - cols
        for dy in (-1, 0, 1):
            for g in range(groups):
                b, low = g // per, (g % per) * width
                right = edge_in[kind, dy + 1, 0, b * PACK : (b + 1) * PACK, :]
                left = edge_in[kind, dy + 1, 1, b * PACK : (b + 1) * PACK, :]
                both = jnp.where(within(0, width), place(right, -low), place(left, apart - low))
                halo[kind, dy + 1, g * PACK : (g + 1) * PACK, :] = both

    lane_ch = lax.broadcasted_iota(jnp.int32, (ch, lanes), 1)
    at_halo = ((lane_ch >= cols) & (lane_ch < cols + 2)) | (lane_ch >= lanes - 2)

    def shifts(layer, slot, j, v):
        x[layer, slot, j, 0:ch] = place(v, 1)
        x[layer, slot, j, ch : 2 * ch] = v
        x[layer, slot, j, 2 * ch : 3 * ch] = place(v, -1)

    def spread(layer, slot, lines):
        for j in lines:
            side = 0 if j == 0 else 1
            if j in (0, rows + 1):
                v = rows_in[layer, side, slot]
            elif slot < 2:
                v = past[layer, slot, j - 1]
            else:
                v = plane[layer, slot - 2, j - 1]
            if layer == 0:
                kind = PAST if slot < 2 else NOW
                dy = 1 if j == 0 else -1 if j == rows + 1 else 0
                f = slot + frames - 2 if slot < 2 else slot - 2
                index = 2 * (f * rows + (line(dy) if dy else j - 1))
                v = jnp.where(at_halo, place(halo[kind, dy + 1], cols - index), v)
            shifts(layer, slot, j, v)

    def conv(layer, terms):
        left, right = [], []
        for slot, p in terms:
            left += [wt[layer, p, c] for c in range(wt.shape[2])]
            for q in range(3):
                right.append(jnp.concatenate([x[layer, slot, q + r] for r in range(rows)], axis=1))
            if padded > taps:
                right.append(zero[...])
        lhs = jnp.concatenate(left, axis=1)
        rhs = jnp.concatenate(right, axis=0)
        return jnp.dot(lhs, rhs, preferred_element_type=f32)

    keep = (lane < cols) | ((lane == cols) & (gx < size["gx"] - 1)) | ((lane == lanes - 1) & (gx > 0))

    def middle(f, total):
        for row in range(rows):
            value = total[:, row * lanes : (row + 1) * lanes] + vec[1]
            value = activate(value.astype(bf16).astype(f32), vec[2])
            value = jnp.where(keep, value, 0.0).astype(bf16)
            plane[1, f, row] = value
            shifts(1, f + 2, row + 1, value)

    def send_middle(f):
        for side in range(2):
            pl.when(to_side[side])(rows2_copy(f, side).start)
        if f >= frames - 2:
            @pl.when(has_next)
            def _():
                for o in range(rows):
                    past2_copy(f - frames + 2, o).start()

    def finish(f, total):
        for row in range(rows):
            value = total[:, row * lanes : row * lanes + cols] + vec[3, :, 0:cols]
            out[f, row] = (value + fin[f, row].astype(f32)).astype(bf16)

    every = range(rows + 2)
    for side in range(2):
        pl.when(from_side[side])(rows1_copy(side).wait_recv)
    receive_edges(NOW)
    for slot in range(2, 5):
        spread(0, slot, every)
    for f in range(2, frames):
        if f > 2:
            spread(0, f + 2, every)
        middle(f, conv(0, [(f + p, p) for p in range(3)]))
        send_middle(f)

    def pass_on(wait, copies):
        @pl.when(has_past)
        def _():
            wait(0)
            for side in range(2):
                for copy in copies(side):
                    pl.when(to_side[side] & (turn(0) == line(1 - 2 * side)))(copy.start)

    def pass_rest(wait, copies):
        @pl.when(has_past)
        def _():
            for o in range(1, rows):
                wait(o)
            for side in range(2) if size["gy"] > 2 else ():
                for copy in copies(side):
                    pl.when(to_side[side] & (turn(0) != line(1 - 2 * side)))(copy.start)

    wait1 = lambda o: past1_copy(o).wait_recv()
    pass_on(wait1, lambda side: [pass1_copy(side)])
    acc[0] = conv(0, [(2, 2)])
    acc[1] = conv(0, [(2, 1), (3, 2)])
    pass_rest(wait1, lambda side: [pass1_copy(side)])
    for side in range(2):
        pl.when(has_past & from_side[side])(pass1_copy(side).wait_recv)
    receive_edges(PAST)
    for slot in range(2):
        spread(0, slot, every)
    middle(1, acc[1] + conv(0, [(1, 0)]))
    middle(0, acc[0] + conv(0, [(0, 0), (1, 1)]))
    for f in (1, 0):
        send_middle(f)

    def receive_rows2(f):
        for side in range(2):
            pl.when(from_side[side])(rows2_copy(f, side).wait_recv)
        spread(1, f + 2, (0, rows + 1))

    for f in range(2, frames):
        receive_rows2(f)
    acc[2] = conv(1, [(4, 2)])
    acc[3] = conv(1, [(4, 1), (5, 2)])

    for f in (1, 0):
        receive_rows2(f)
    finish(3, acc[3] + conv(1, [(3, 0)]))
    finish(2, acc[2] + conv(1, [(2, 0), (3, 1)]))
    wait2 = [lambda o, i=i: past2_copy(i, o).wait_recv() for i in range(2)]
    pass2 = [lambda side, i=i: [pass2_copy(i, side)] for i in range(2)]
    pass_on(wait2[0], pass2[0])
    acc[1] = conv(1, [(2, 1), (3, 2)])
    acc[0] = conv(1, [(2, 2)])
    pass_on(wait2[1], pass2[1])
    for i in range(2):
        pass_rest(wait2[i], pass2[i])
        for side in range(2):
            pl.when(has_past & from_side[side])(pass2_copy(i, side).wait_recv)
        spread(1, i, every)
    finish(1, acc[1] + conv(1, [(1, 0)]))
    finish(0, acc[0] + conv(1, [(0, 0), (1, 1)]))

    for kind in (NOW, PAST):
        for dy in (-1, 0, 1):
            for dx in (-1, 1):
                pl.when(at(kind, dy, dx)[0])(edge_copy(kind, dy, dx).wait_send)
    for side in range(2):
        @pl.when(to_side[side])
        def _():
            rows1_copy(side).wait_send()
            for f in range(frames):
                rows2_copy(f, side).wait_send()

        @pl.when(to_side[side] & has_past)
        def _():
            pass1_copy(side).wait_send()
            for i in range(2):
                pass2_copy(i, side).wait_send()

    @pl.when(has_next)
    def _():
        for o in range(rows):
            past1_copy(o).wait_send()
            for i in range(2):
                past2_copy(i, o).wait_send()


def local(features, gain_first, kernel_first, bias_first, gain_second, kernel_second, bias_second):
    frames, rows, cols, ch = features.shape
    lanes = -(-(cols + 4) // 128) * 128
    whole = max(MATMUL, lanes)
    padded = -(-9 * ch // whole) * whole
    per = lanes // (2 * frames * rows)
    blocks = -(-(ch // PACK) // per)
    hbm = pl.BlockSpec(memory_space=pl.ANY)
    bf16, f32 = jnp.bfloat16, jnp.float32
    messages = len(message_numbers(frames, rows))
    dma = pltpu.SemaphoreType.DMA
    result = pl.pallas_call(
        block_kernel,
        out_shape=pltpu.VMEM((frames, rows, ch, cols), bf16),
        in_specs=[hbm] * 7,
        out_specs=pl.BlockSpec(memory_space=pltpu.VMEM),
        scratch_shapes=[
            pltpu.VMEM((frames, rows, ch, cols), bf16),
            pltpu.VMEM((2, 27 * ch, ch), bf16),
            pltpu.VMEM((2, 3, padded // lanes, ch, lanes), bf16),
            pltpu.VMEM((4, 1, ch), f32),
            pltpu.VMEM((4, ch, lanes), f32),
            pltpu.VMEM((2, frames, rows, ch, lanes), bf16),
            pltpu.VMEM((2, 2, rows, ch, lanes), bf16),
            pltpu.VMEM((2, 2, frames + 2, ch, lanes), bf16),
            pltpu.VMEM((2, blocks * PACK, lanes), bf16),
            pltpu.VMEM((2, 3, 2, blocks * PACK, lanes), bf16),
            pltpu.VMEM((2, 3, ch, lanes), bf16),
            pltpu.VMEM((2, frames + 2, rows + 2, 3 * ch, lanes), bf16),
            pltpu.VMEM((max(padded - 9 * ch, PACK), rows * lanes), bf16),
            pltpu.VMEM((frames, ch, rows * lanes), f32),
            dma((4,)),
            dma((frames,)),
            dma((2, 3)),
            dma((messages,)),
            dma((messages,)),
        ],
        compiler_params=pltpu.CompilerParams(
            collective_id=0, has_side_effects=True, vmem_limit_bytes=56 * 1024 * 1024
        ),
        name="residual_block",
    )(
        jnp.swapaxes(features, 2, 3),
        gain_first.reshape(1, ch),
        bias_first.reshape(1, ch),
        gain_second.reshape(1, ch),
        bias_second.reshape(1, ch),
        kernel_first.reshape(27 * ch, ch),
        kernel_second.reshape(27 * ch, ch),
    )
    return jnp.swapaxes(result, 2, 3)


def solution(mesh):
    placed = (P("ta", "gy", "gx", None), P(), P(), P(), P(), P(), P())
    return jax.shard_map(
        local, mesh=mesh, in_specs=placed, out_specs=P("ta", "gy", "gx", None), check_vma=False
    )
```

```python
import jax
import jax.numpy as jnp
from jax import lax
from jax.experimental import pallas as pl
from jax.experimental.pallas import tpu as pltpu
from jax.sharding import PartitionSpec as P

epsilon = 1e-06
AXES = ("ta", "gy", "gx")
NOW, PAST = 0, 1
PACK = 16
MATMUL = 256


def activate(field, gain):
    meansq = jnp.mean(field * field, axis=0, keepdims=True)
    u = field * lax.rsqrt(meansq + epsilon) * gain
    return u / (1.0 + jnp.exp(-u))


def message_numbers(frames, rows):
    names = [("edge", dy, dx) for dy in (-1, 0, 1) for dx in (-1, 1)] + [("past_edge",)]
    names += [("rows1", side) for side in range(2)]
    names += [("rows2", f, side) for f in range(frames) for side in range(2)]
    names += [("past1", o) for o in range(rows)]
    names += [("past2", i, o) for i in range(2) for o in range(rows)]
    names += [("pass1", side) for side in range(2)]
    names += [("pass2", i, side) for i in range(2) for side in range(2)]
    return {name: n for n, name in enumerate(names)}


def block_kernel(
    feat, gain1, bias1, gain2, bias2, k1, k2, out,
    fin, raw, wt, vec_raw, vec, plane, past, rows_in, edge_out, edge_in, halo, x, zero, acc,
    vec_sem, in_sem, w_sem, send_sem, recv_sem,
):
    frames, rows, ch, cols = fin.shape
    lanes = plane.shape[-1]
    bf16, f32 = jnp.bfloat16, jnp.float32
    taps = 9 * ch
    padded = wt.shape[2] * lanes
    groups = ch // PACK
    width = 2 * frames * rows
    per = lanes // width
    number = message_numbers(frames, rows)
    me = {a: lax.axis_index(a) for a in AXES}
    size = {a: lax.axis_size(a) for a in AXES}
    ta, gy, gx = (me[a] for a in AXES)

    def at(dt, dy, dx):
        place = {"ta": ta + dt, "gy": gy + dy, "gx": gx + dx}
        ok = None
        for a, d in zip(AXES, (dt, dy, dx)):
            if isinstance(d, int) and d == 0:
                continue
            inside = (place[a] >= 0) & (place[a] < size[a])
            ok = inside if ok is None else ok & inside
        return ok, place

    moves = [(0, dy, dx) for dy in (-1, 0, 1) for dx in (-1, 0, 1) if dy or dx]
    moves += [(1, 0, 0)]
    barrier = pltpu.get_barrier_semaphore()
    expected = jnp.int32(0)
    for dt, dy, dx in moves:
        ok, source = at(-dt, -dy, -dx)

        @pl.when(ok)
        def _():
            pl.semaphore_signal(
                barrier, inc=1, device_id=source, device_id_type=pl.DeviceIdType.MESH
            )

        expected = expected + at(dt, dy, dx)[0].astype(jnp.int32)

    fin_copies = [pltpu.make_async_copy(feat.at[f], fin.at[f], in_sem.at[f]) for f in range(frames)]
    for f in reversed(range(frames)):
        fin_copies[f].start()
    vec_copies = [
        pltpu.make_async_copy(v, vec_raw.at[i], vec_sem.at[i])
        for i, v in enumerate((gain1, bias1, gain2, bias2))
    ]
    for copy in vec_copies:
        copy.start()
    w_copies = [
        [
            pltpu.make_async_copy(
                k.at[pl.ds(p * taps, taps)], raw.at[layer, pl.ds(p * taps, taps)], w_sem.at[layer, p]
            )
            for p in range(3)
        ]
        for layer, k in enumerate((k1, k2))
    ]

    def copy_to(name, src, dst, target):
        n = number[name] if isinstance(name, tuple) else name
        return pltpu.make_async_remote_copy(
            src_ref=src,
            dst_ref=dst,
            send_sem=send_sem.at[n],
            recv_sem=recv_sem.at[n],
            device_id=target,
            device_id_type=pl.DeviceIdType.MESH,
        )

    def edge_copy(dy, dx):
        side = (dx + 1) // 2
        target = at(0, dy, dx)[1]
        return copy_to(("edge", dy, dx), edge_out.at[side], edge_in.at[NOW, dy + 1, side], target)

    def past_edge_copy():
        return copy_to(("past_edge",), edge_in.at[NOW], edge_in.at[PAST], at(1, 0, 0)[1])

    def line(dy):
        return rows - 1 if dy > 0 else 0

    def rows1_copy(side):
        dy = 1 if side == 0 else -1
        src = plane.at[0, :, line(dy)]
        return copy_to(("rows1", side), src, rows_in.at[0, side, pl.ds(2, frames)], at(0, dy, 0)[1])

    def rows2_copy(f, side):
        dy = 1 if side == 0 else -1
        src = plane.at[1, f, line(dy)]
        return copy_to(("rows2", f, side), src, rows_in.at[1, side, 2 + f], at(0, dy, 0)[1])

    def turn(o):
        return jnp.where(gy == 0, rows - 1 - o, o)

    def past1_copy(o):
        r = turn(o)
        src = plane.at[0, pl.ds(frames - 2, 2), r]
        return copy_to(("past1", o), src, past.at[0, :, r], at(1, 0, 0)[1])

    def past2_copy(i, o):
        r = turn(o)
        return copy_to(("past2", i, o), plane.at[1, frames - 2 + i, r], past.at[1, i, r], at(1, 0, 0)[1])

    def pass1_copy(side):
        dy = 1 if side == 0 else -1
        dst = rows_in.at[0, side, pl.ds(0, 2)]
        return copy_to(("pass1", side), past.at[0, :, line(dy)], dst, at(0, dy, 0)[1])

    def pass2_copy(i, side):
        dy = 1 if side == 0 else -1
        dst = rows_in.at[1, side, i]
        return copy_to(("pass2", i, side), past.at[1, i, line(dy)], dst, at(0, dy, 0)[1])

    has_past, has_next = ta > 0, ta < size["ta"] - 1
    from_side = (gy > 0, gy < size["gy"] - 1)
    to_side = (gy < size["gy"] - 1, gy > 0)

    for side in range(2):
        @pl.when(jnp.logical_not(from_side[side]))
        def _():
            rows_in[:, side] = jnp.zeros((2, frames + 2, ch, lanes), bf16)

    @pl.when(jnp.logical_not(has_past))
    def _():
        past[...] = jnp.zeros_like(past)
        rows_in[:, :, 0:2] = jnp.zeros((2, 2, 2, ch, lanes), bf16)
        edge_in[PAST] = jnp.zeros(edge_in.shape[1:], bf16)

    for dy in (-1, 0, 1):
        for dx in (-1, 1):
            @pl.when(jnp.logical_not(at(0, -dy, -dx)[0]))
            def _():
                edge_in[NOW, dy + 1, (dx + 1) // 2] = jnp.zeros(edge_in.shape[3:], bf16)

    plane[0] = jnp.zeros(plane.shape[1:], bf16)
    zero[...] = jnp.zeros_like(zero)
    if padded > taps:
        for layer in range(2):
            for p in range(3):
                for low in range(taps // lanes * lanes, padded, lanes):
                    wt[layer, p, low // lanes] = jnp.zeros((ch, lanes), bf16)
    for i, copy in enumerate(vec_copies):
        copy.wait()
        vec[i] = jnp.broadcast_to(vec_raw[i], (lanes, ch)).T

    lane = lax.broadcasted_iota(jnp.int32, (1, lanes), 1)

    for copy in fin_copies:
        copy.wait()
    for p in (2, 1, 0):
        w_copies[0][p].start()
    for f in reversed(range(frames)):
        for row in range(rows):
            value = activate(fin[f, row].astype(f32), vec[0, :, 0:cols])
            plane[0, f, row, :, 0:cols] = value.astype(bf16)

    def place(v, shift):
        shift = shift % lanes
        return pltpu.roll(v, shift, 1) if shift else v

    lane_pack = lax.broadcasted_iota(jnp.int32, (PACK, lanes), 1)

    def within(low, count):
        return (lane_pack >= low) & (lane_pack < low + count)

    for side in range(2):
        first_col = 0 if side == 0 else cols - 2
        for b in range(edge_out.shape[1] // PACK):
            total = jnp.zeros((PACK, lanes), bf16)
            for f in range(frames):
                for row in range(rows):
                    slot = 2 * (f * rows + row)
                    for g in range(b * per, min(groups, (b + 1) * per)):
                        low = (g - b * per) * width + slot
                        v = plane[0, f, row, g * PACK : (g + 1) * PACK, :]
                        total = jnp.where(within(low, 2), place(v, low - first_col), total)
            edge_out[side, b * PACK : (b + 1) * PACK, :] = total

    pl.semaphore_wait(barrier, expected)
    for dy in (0, -1, 1):
        for dx in (-1, 1):
            pl.when(at(0, dy, dx)[0])(edge_copy(dy, dx).start)
    for side in range(2):
        pl.when(to_side[side])(rows1_copy(side).start)

    @pl.when(has_next)
    def _():
        for o in range(rows):
            past1_copy(o).start()

    for p in (2, 1, 0):
        w_copies[1][p].start()

    def transpose_weights(layer):
        for p in (2, 1, 0):
            w_copies[layer][p].wait()
            for low in range(0, taps, lanes):
                count = min(lanes, taps - low)
                block = raw[layer, p * taps + low : p * taps + low + count, :]
                wt[layer, p, low // lanes, :, 0:count] = block.T

    transpose_weights(0)
    transpose_weights(1)

    def receive_edges(kind):
        if kind == PAST:
            pl.when(has_past)(past_edge_copy().wait_recv)
        else:
            for dy in (-1, 0, 1):
                for dx in (-1, 1):
                    pl.when(at(0, -dy, -dx)[0])(edge_copy(dy, dx).wait_recv)
            pl.when(has_next)(past_edge_copy().start)
        apart = lanes - 2 - cols
        for dy in (-1, 0, 1):
            for g in range(groups):
                b, low = g // per, (g % per) * width
                right = edge_in[kind, dy + 1, 0, b * PACK : (b + 1) * PACK, :]
                left = edge_in[kind, dy + 1, 1, b * PACK : (b + 1) * PACK, :]
                both = jnp.where(within(0, width), place(right, -low), place(left, apart - low))
                halo[kind, dy + 1, g * PACK : (g + 1) * PACK, :] = both

    lane_ch = lax.broadcasted_iota(jnp.int32, (ch, lanes), 1)
    at_halo = ((lane_ch >= cols) & (lane_ch < cols + 2)) | (lane_ch >= lanes - 2)

    def shifts(layer, slot, j, v):
        x[layer, slot, j, 0:ch] = place(v, 1)
        x[layer, slot, j, ch : 2 * ch] = v
        x[layer, slot, j, 2 * ch : 3 * ch] = place(v, -1)

    def spread(layer, slot, lines):
        for j in lines:
            side = 0 if j == 0 else 1
            if j in (0, rows + 1):
                v = rows_in[layer, side, slot]
            elif slot < 2:
                v = past[layer, slot, j - 1]
            else:
                v = plane[layer, slot - 2, j - 1]
            if layer == 0:
                kind = PAST if slot < 2 else NOW
                dy = 1 if j == 0 else -1 if j == rows + 1 else 0
                f = slot + frames - 2 if slot < 2 else slot - 2
                index = 2 * (f * rows + (line(dy) if dy else j - 1))
                v = jnp.where(at_halo, place(halo[kind, dy + 1], cols - index), v)
            shifts(layer, slot, j, v)

    def conv(layer, terms):
        left, right = [], []
        for slot, p in terms:
            left += [wt[layer, p, c] for c in range(wt.shape[2])]
            for q in range(3):
                right.append(jnp.concatenate([x[layer, slot, q + r] for r in range(rows)], axis=1))
            if padded > taps:
                right.append(zero[...])
        lhs = jnp.concatenate(left, axis=1)
        rhs = jnp.concatenate(right, axis=0)
        return jnp.dot(lhs, rhs, preferred_element_type=f32)

    keep = (lane < cols) | ((lane == cols) & (gx < size["gx"] - 1)) | ((lane == lanes - 1) & (gx > 0))

    def middle(f, total):
        for row in range(rows):
            value = total[:, row * lanes : (row + 1) * lanes] + vec[1]
            value = activate(value.astype(bf16).astype(f32), vec[2])
            value = jnp.where(keep, value, 0.0).astype(bf16)
            plane[1, f, row] = value
            shifts(1, f + 2, row + 1, value)

    def send_middle(f):
        for side in range(2):
            pl.when(to_side[side])(rows2_copy(f, side).start)
        if f >= frames - 2:
            @pl.when(has_next)
            def _():
                for o in range(rows):
                    past2_copy(f - frames + 2, o).start()

    def finish(f, total):
        for row in range(rows):
            value = total[:, row * lanes : row * lanes + cols] + vec[3, :, 0:cols]
            out[f, row] = (value + fin[f, row].astype(f32)).astype(bf16)

    every = range(rows + 2)
    for side in range(2):
        pl.when(from_side[side])(rows1_copy(side).wait_recv)
    receive_edges(NOW)
    def pass_on(wait, copies):
        @pl.when(has_past)
        def _():
            wait(0)
            for side in range(2):
                for copy in copies(side):
                    pl.when(to_side[side] & (turn(0) == line(1 - 2 * side)))(copy.start)

    def pass_rest(wait, copies):
        @pl.when(has_past)
        def _():
            for o in range(1, rows):
                wait(o)
            for side in range(2) if size["gy"] > 2 else ():
                for copy in copies(side):
                    pl.when(to_side[side] & (turn(0) != line(1 - 2 * side)))(copy.start)

    wait1 = lambda o: past1_copy(o).wait_recv()
    pass1 = lambda side: [pass1_copy(side)]
    wait2 = [lambda o, i=i: past2_copy(i, o).wait_recv() for i in range(2)]
    pass2 = [lambda side, i=i: [pass2_copy(i, side)] for i in range(2)]

    def wait_rows2(f):
        for side in range(2):
            pl.when(from_side[side])(rows2_copy(f, side).wait_recv)

    outer = (0, rows + 1)
    for slot in range(2, 5):
        spread(0, slot, every)
    middle(2, conv(0, [(2, 0), (3, 1), (4, 2)]))
    send_middle(2)
    pass_on(wait1, pass1)
    spread(0, 5, every)
    middle(3, conv(0, [(3, 0), (4, 1), (5, 2)]))
    send_middle(3)
    pass_rest(wait1, pass1)
    for side in range(2):
        pl.when(has_past & from_side[side])(pass1_copy(side).wait_recv)
    receive_edges(PAST)
    for slot in range(2):
        spread(0, slot, every)
    middle(1, conv(0, [(3, 2), (2, 1), (1, 0)]))
    middle(0, conv(0, [(2, 2), (1, 1), (0, 0)]))
    for f in (1, 0):
        send_middle(f)

    for f in (2, 3):
        wait_rows2(f)
    for slot in (4, 5):
        spread(1, slot, outer)
    acc[3] = conv(1, [(4, 1), (5, 2)])
    acc[2] = conv(1, [(4, 2)])
    for f in (1, 0):
        wait_rows2(f)
    for slot in (3, 2):
        spread(1, slot, outer)
    pass_on(wait2[0], pass2[0])
    finish(3, acc[3] + conv(1, [(3, 0)]))
    finish(2, acc[2] + conv(1, [(3, 1), (2, 0)]))
    pass_on(wait2[1], pass2[1])
    acc[1] = conv(1, [(3, 2), (2, 1)])
    acc[0] = conv(1, [(2, 2)])
    for i in range(2):
        pass_rest(wait2[i], pass2[i])
    for i in range(2):
        for side in range(2):
            pl.when(has_past & from_side[side])(pass2_copy(i, side).wait_recv)
    for i in (1, 0):
        spread(1, i, every)
    finish(1, acc[1] + conv(1, [(1, 0)]))
    finish(0, acc[0] + conv(1, [(1, 1), (0, 0)]))

    for dy in (-1, 0, 1):
        for dx in (-1, 1):
            pl.when(at(0, dy, dx)[0])(edge_copy(dy, dx).wait_send)
    for side in range(2):
        @pl.when(to_side[side])
        def _():
            rows1_copy(side).wait_send()
            for f in range(frames):
                rows2_copy(f, side).wait_send()

        @pl.when(to_side[side] & has_past)
        def _():
            pass1_copy(side).wait_send()
            for i in range(2):
                pass2_copy(i, side).wait_send()

    @pl.when(has_next)
    def _():
        past_edge_copy().wait_send()
        for o in range(rows):
            past1_copy(o).wait_send()
            for i in range(2):
                past2_copy(i, o).wait_send()


def local(features, gain_first, kernel_first, bias_first, gain_second, kernel_second, bias_second):
    frames, rows, cols, ch = features.shape
    lanes = -(-(cols + 4) // 128) * 128
    whole = max(MATMUL, lanes)
    padded = -(-9 * ch // whole) * whole
    per = lanes // (2 * frames * rows)
    blocks = -(-(ch // PACK) // per)
    hbm = pl.BlockSpec(memory_space=pl.ANY)
    bf16, f32 = jnp.bfloat16, jnp.float32
    messages = len(message_numbers(frames, rows))
    dma = pltpu.SemaphoreType.DMA
    result = pl.pallas_call(
        block_kernel,
        out_shape=pltpu.VMEM((frames, rows, ch, cols), bf16),
        in_specs=[hbm] * 7,
        out_specs=pl.BlockSpec(memory_space=pltpu.VMEM),
        scratch_shapes=[
            pltpu.VMEM((frames, rows, ch, cols), bf16),
            pltpu.VMEM((2, 27 * ch, ch), bf16),
            pltpu.VMEM((2, 3, padded // lanes, ch, lanes), bf16),
            pltpu.VMEM((4, 1, ch), f32),
            pltpu.VMEM((4, ch, lanes), f32),
            pltpu.VMEM((2, frames, rows, ch, lanes), bf16),
            pltpu.VMEM((2, 2, rows, ch, lanes), bf16),
            pltpu.VMEM((2, 2, frames + 2, ch, lanes), bf16),
            pltpu.VMEM((2, blocks * PACK, lanes), bf16),
            pltpu.VMEM((2, 3, 2, blocks * PACK, lanes), bf16),
            pltpu.VMEM((2, 3, ch, lanes), bf16),
            pltpu.VMEM((2, frames + 2, rows + 2, 3 * ch, lanes), bf16),
            pltpu.VMEM((max(padded - 9 * ch, PACK), rows * lanes), bf16),
            pltpu.VMEM((frames, ch, rows * lanes), f32),
            dma((4,)),
            dma((frames,)),
            dma((2, 3)),
            dma((messages,)),
            dma((messages,)),
        ],
        compiler_params=pltpu.CompilerParams(
            collective_id=0, has_side_effects=True, vmem_limit_bytes=56 * 1024 * 1024
        ),
        name="residual_block",
    )(
        jnp.swapaxes(features, 2, 3),
        gain_first.reshape(1, ch),
        bias_first.reshape(1, ch),
        gain_second.reshape(1, ch),
        bias_second.reshape(1, ch),
        kernel_first.reshape(27 * ch, ch),
        kernel_second.reshape(27 * ch, ch),
    )
    return jnp.swapaxes(result, 2, 3)


def solution(mesh):
    placed = (P("ta", "gy", "gx", None), P(), P(), P(), P(), P(), P())
    return jax.shard_map(
        local, mesh=mesh, in_specs=placed, out_specs=P("ta", "gy", "gx", None), check_vma=False
    )
```

```python
import jax
import jax.numpy as jnp
from jax import lax
from jax.experimental import pallas as pl
from jax.experimental.pallas import tpu as pltpu
from jax.sharding import PartitionSpec as P

epsilon = 1e-06
AXES = ("ta", "gy", "gx")
NOW, PAST = 0, 1
PACK = 16
MATMUL = 256


def activate(field, gain):
    meansq = jnp.mean(field * field, axis=0, keepdims=True)
    u = field * lax.rsqrt(meansq + epsilon) * gain
    return u / (1.0 + jnp.exp(-u))


def message_numbers(frames, rows):
    names = [("edge", dy, dx) for dy in (-1, 0, 1) for dx in (-1, 1)]
    names += [("past_edge", dy) for dy in (-1, 0, 1)]
    names += [("rows1", side) for side in range(2)]
    names += [("rows2", f, side) for f in range(frames) for side in range(2)]
    names += [("past1", o) for o in range(rows)]
    names += [("past2", i, o) for i in range(2) for o in range(rows)]
    names += [("pass1", side) for side in range(2)]
    names += [("pass2", i, side) for i in range(2) for side in range(2)]
    return {name: n for n, name in enumerate(names)}


def block_kernel(
    feat, gain1, bias1, gain2, bias2, k1, k2, out,
    fin, raw, wt, vec_raw, vec, plane, past, rows_in, edge_out, edge_in, halo, x, zero, acc,
    vec_sem, in_sem, w_sem, send_sem, recv_sem,
):
    frames, rows, ch, cols = fin.shape
    lanes = plane.shape[-1]
    bf16, f32 = jnp.bfloat16, jnp.float32
    taps = 9 * ch
    padded = wt.shape[2] * lanes
    groups = ch // PACK
    width = 2 * frames * rows
    per = lanes // width
    number = message_numbers(frames, rows)
    me = {a: lax.axis_index(a) for a in AXES}
    size = {a: lax.axis_size(a) for a in AXES}
    ta, gy, gx = (me[a] for a in AXES)

    def at(dt, dy, dx):
        place = {"ta": ta + dt, "gy": gy + dy, "gx": gx + dx}
        ok = None
        for a, d in zip(AXES, (dt, dy, dx)):
            if isinstance(d, int) and d == 0:
                continue
            inside = (place[a] >= 0) & (place[a] < size[a])
            ok = inside if ok is None else ok & inside
        return ok, place

    moves = [(0, dy, dx) for dy in (-1, 0, 1) for dx in (-1, 0, 1) if dy or dx]
    moves += [(1, 0, 0)]
    barrier = pltpu.get_barrier_semaphore()
    expected = jnp.int32(0)
    for dt, dy, dx in moves:
        ok, source = at(-dt, -dy, -dx)

        @pl.when(ok)
        def _():
            pl.semaphore_signal(
                barrier, inc=1, device_id=source, device_id_type=pl.DeviceIdType.MESH
            )

        expected = expected + at(dt, dy, dx)[0].astype(jnp.int32)

    fin_copies = [pltpu.make_async_copy(feat.at[f], fin.at[f], in_sem.at[f]) for f in range(frames)]
    for f in reversed(range(frames)):
        fin_copies[f].start()
    vec_copies = [
        pltpu.make_async_copy(v, vec_raw.at[i], vec_sem.at[i])
        for i, v in enumerate((gain1, bias1, gain2, bias2))
    ]
    for copy in vec_copies:
        copy.start()
    w_copies = [
        [
            pltpu.make_async_copy(
                k.at[pl.ds(p * taps, taps)], raw.at[layer, pl.ds(p * taps, taps)], w_sem.at[layer, p]
            )
            for p in range(3)
        ]
        for layer, k in enumerate((k1, k2))
    ]

    def copy_to(name, src, dst, target):
        n = number[name] if isinstance(name, tuple) else name
        return pltpu.make_async_remote_copy(
            src_ref=src,
            dst_ref=dst,
            send_sem=send_sem.at[n],
            recv_sem=recv_sem.at[n],
            device_id=target,
            device_id_type=pl.DeviceIdType.MESH,
        )

    def edge_copy(dy, dx):
        side = (dx + 1) // 2
        target = at(0, dy, dx)[1]
        return copy_to(("edge", dy, dx), edge_out.at[side], edge_in.at[NOW, dy + 1, side], target)

    def past_edge_copy(dy):
        src, dst = edge_in.at[NOW, dy + 1], edge_in.at[PAST, dy + 1]
        return copy_to(("past_edge", dy), src, dst, at(1, 0, 0)[1])

    def past_edges(has, act):
        for dy in (0, -1, 1):
            pl.when(has & from_side[0 if dy > 0 else 1] if dy else has)(act(past_edge_copy(dy)))

    def line(dy):
        return rows - 1 if dy > 0 else 0

    def rows1_copy(side):
        dy = 1 if side == 0 else -1
        src = plane.at[0, :, line(dy)]
        return copy_to(("rows1", side), src, rows_in.at[0, side, pl.ds(2, frames)], at(0, dy, 0)[1])

    def rows2_copy(f, side):
        dy = 1 if side == 0 else -1
        src = plane.at[1, f, line(dy)]
        return copy_to(("rows2", f, side), src, rows_in.at[1, side, 2 + f], at(0, dy, 0)[1])

    def turn(o):
        return jnp.where(gy == 0, rows - 1 - o, o)

    def past1_copy(o):
        r = turn(o)
        src = plane.at[0, pl.ds(frames - 2, 2), r]
        return copy_to(("past1", o), src, past.at[0, :, r], at(1, 0, 0)[1])

    def past2_copy(i, o):
        r = turn(o)
        return copy_to(("past2", i, o), plane.at[1, frames - 2 + i, r], past.at[1, i, r], at(1, 0, 0)[1])

    def pass1_copy(side):
        dy = 1 if side == 0 else -1
        dst = rows_in.at[0, side, pl.ds(0, 2)]
        return copy_to(("pass1", side), past.at[0, :, line(dy)], dst, at(0, dy, 0)[1])

    def pass2_copy(i, side):
        dy = 1 if side == 0 else -1
        dst = rows_in.at[1, side, i]
        return copy_to(("pass2", i, side), past.at[1, i, line(dy)], dst, at(0, dy, 0)[1])

    has_past, has_next = ta > 0, ta < size["ta"] - 1
    from_side = (gy > 0, gy < size["gy"] - 1)
    to_side = (gy < size["gy"] - 1, gy > 0)

    for side in range(2):
        @pl.when(jnp.logical_not(from_side[side]))
        def _():
            rows_in[:, side] = jnp.zeros((2, frames + 2, ch, lanes), bf16)
            edge_in[PAST, 2 - 2 * side] = jnp.zeros(edge_in.shape[2:], bf16)

    @pl.when(jnp.logical_not(has_past))
    def _():
        past[...] = jnp.zeros_like(past)
        rows_in[:, :, 0:2] = jnp.zeros((2, 2, 2, ch, lanes), bf16)
        edge_in[PAST] = jnp.zeros(edge_in.shape[1:], bf16)

    for dy in (-1, 0, 1):
        for dx in (-1, 1):
            @pl.when(jnp.logical_not(at(0, -dy, -dx)[0]))
            def _():
                edge_in[NOW, dy + 1, (dx + 1) // 2] = jnp.zeros(edge_in.shape[3:], bf16)

    plane[0] = jnp.zeros(plane.shape[1:], bf16)
    zero[...] = jnp.zeros_like(zero)
    if padded > taps:
        for layer in range(2):
            for p in range(3):
                for low in range(taps // lanes * lanes, padded, lanes):
                    wt[layer, p, low // lanes] = jnp.zeros((ch, lanes), bf16)
    for i, copy in enumerate(vec_copies):
        copy.wait()
        vec[i] = jnp.broadcast_to(vec_raw[i], (lanes, ch)).T

    lane = lax.broadcasted_iota(jnp.int32, (1, lanes), 1)

    for copy in fin_copies:
        copy.wait()
    for p in (2, 1, 0):
        w_copies[0][p].start()
    for f in reversed(range(frames)):
        for row in range(rows):
            value = activate(fin[f, row].astype(f32), vec[0, :, 0:cols])
            plane[0, f, row, :, 0:cols] = value.astype(bf16)

    def place(v, shift):
        shift = shift % lanes
        return pltpu.roll(v, shift, 1) if shift else v

    lane_pack = lax.broadcasted_iota(jnp.int32, (PACK, lanes), 1)

    def within(low, count):
        return (lane_pack >= low) & (lane_pack < low + count)

    for side in range(2):
        first_col = 0 if side == 0 else cols - 2
        for b in range(edge_out.shape[1] // PACK):
            total = jnp.zeros((PACK, lanes), bf16)
            for f in range(frames):
                for row in range(rows):
                    slot = 2 * (f * rows + row)
                    for g in range(b * per, min(groups, (b + 1) * per)):
                        low = (g - b * per) * width + slot
                        v = plane[0, f, row, g * PACK : (g + 1) * PACK, :]
                        total = jnp.where(within(low, 2), place(v, low - first_col), total)
            edge_out[side, b * PACK : (b + 1) * PACK, :] = total

    pl.semaphore_wait(barrier, expected)
    for dy in (0, -1, 1):
        for dx in (-1, 1):
            pl.when(at(0, dy, dx)[0])(edge_copy(dy, dx).start)
    for side in range(2):
        pl.when(to_side[side])(rows1_copy(side).start)

    @pl.when(has_next)
    def _():
        for o in range(rows):
            past1_copy(o).start()

    for p in (2, 1, 0):
        w_copies[1][p].start()

    def transpose_weights(layer):
        for p in (2, 1, 0):
            w_copies[layer][p].wait()
            for low in range(0, taps, lanes):
                count = min(lanes, taps - low)
                block = raw[layer, p * taps + low : p * taps + low + count, :]
                wt[layer, p, low // lanes, :, 0:count] = block.T

    transpose_weights(0)
    transpose_weights(1)

    def receive_edges(kind):
        if kind == PAST:
            past_edges(has_past, lambda copy: copy.wait_recv)
        else:
            for dy in (-1, 0, 1):
                for dx in (-1, 1):
                    pl.when(at(0, -dy, -dx)[0])(edge_copy(dy, dx).wait_recv)
            past_edges(has_next, lambda copy: copy.start)
        apart = lanes - 2 - cols
        for dy in (-1, 0, 1):
            for g in range(groups):
                b, low = g // per, (g % per) * width
                right = edge_in[kind, dy + 1, 0, b * PACK : (b + 1) * PACK, :]
                left = edge_in[kind, dy + 1, 1, b * PACK : (b + 1) * PACK, :]
                both = jnp.where(within(0, width), place(right, -low), place(left, apart - low))
                halo[kind, dy + 1, g * PACK : (g + 1) * PACK, :] = both

    lane_ch = lax.broadcasted_iota(jnp.int32, (ch, lanes), 1)
    at_halo = ((lane_ch >= cols) & (lane_ch < cols + 2)) | (lane_ch >= lanes - 2)

    def shifts(layer, slot, j, values):
        low, high = j * lanes, (j + len(values)) * lanes
        for r in range(3):
            moved = [place(v, 1 - r) for v in values]
            wide = moved[0] if len(moved) == 1 else jnp.concatenate(moved, axis=1)
            x[layer, slot, r * ch : (r + 1) * ch, low:high] = wide

    def gather(layer, slot, lines):
        values = []
        for j in lines:
            side = 0 if j == 0 else 1
            if j in (0, rows + 1):
                v = rows_in[layer, side, slot]
            elif slot < 2:
                v = past[layer, slot, j - 1]
            else:
                v = plane[layer, slot - 2, j - 1]
            if layer == 0:
                kind = PAST if slot < 2 else NOW
                dy = 1 if j == 0 else -1 if j == rows + 1 else 0
                f = slot + frames - 2 if slot < 2 else slot - 2
                index = 2 * (f * rows + (line(dy) if dy else j - 1))
                v = jnp.where(at_halo, place(halo[kind, dy + 1], cols - index), v)
            values.append(v)
        return values

    def spread(layer, slot, lines):
        if len(lines) == rows + 2 and rows % 2 == 0:
            for j in range(0, rows + 2, 2):
                shifts(layer, slot, j, gather(layer, slot, (j, j + 1)))
        else:
            for j in lines:
                shifts(layer, slot, j, gather(layer, slot, (j,)))

    def conv(layer, terms):
        left, right = [], []
        for slot, p in terms:
            left += [wt[layer, p, c] for c in range(wt.shape[2])]
            for q in range(3):
                right.append(x[layer, slot, :, q * lanes : (q + rows) * lanes])
            if padded > taps:
                right.append(zero[...])
        lhs = jnp.concatenate(left, axis=1)
        rhs = jnp.concatenate(right, axis=0)
        return jnp.dot(lhs, rhs, preferred_element_type=f32)

    keep = (lane < cols) | ((lane == cols) & (gx < size["gx"] - 1)) | ((lane == lanes - 1) & (gx > 0))

    def middle(f, total):
        values = []
        for row in range(rows):
            value = total[:, row * lanes : (row + 1) * lanes] + vec[1]
            value = activate(value.astype(bf16).astype(f32), vec[2])
            value = jnp.where(keep, value, 0.0).astype(bf16)
            plane[1, f, row] = value
            values.append(value)
        shifts(1, f + 2, 1, values)

    def send_middle(f):
        for side in range(2):
            pl.when(to_side[side])(rows2_copy(f, side).start)
        if f >= frames - 2:
            @pl.when(has_next)
            def _():
                for o in range(rows):
                    past2_copy(f - frames + 2, o).start()

    def finish(f, total):
        for row in range(rows):
            value = total[:, row * lanes : row * lanes + cols] + vec[3, :, 0:cols]
            out[f, row] = (value + fin[f, row].astype(f32)).astype(bf16)

    every = range(rows + 2)
    for side in range(2):
        pl.when(from_side[side])(rows1_copy(side).wait_recv)
    receive_edges(NOW)
    def pass_on(wait, copies):
        @pl.when(has_past)
        def _():
            wait(0)
            for side in range(2):
                for copy in copies(side):
                    pl.when(to_side[side] & (turn(0) == line(1 - 2 * side)))(copy.start)

    def pass_rest(wait, copies):
        @pl.when(has_past)
        def _():
            for o in range(1, rows):
                wait(o)
            for side in range(2) if size["gy"] > 2 else ():
                for copy in copies(side):
                    pl.when(to_side[side] & (turn(0) != line(1 - 2 * side)))(copy.start)

    wait1 = lambda o: past1_copy(o).wait_recv()
    pass1 = lambda side: [pass1_copy(side)]
    wait2 = [lambda o, i=i: past2_copy(i, o).wait_recv() for i in range(2)]
    pass2 = [lambda side, i=i: [pass2_copy(i, side)] for i in range(2)]

    def wait_rows2(f):
        for side in range(2):
            pl.when(from_side[side])(rows2_copy(f, side).wait_recv)

    outer = (0, rows + 1)
    for slot in range(2, 5):
        spread(0, slot, every)
    middle(2, conv(0, [(2, 0), (3, 1), (4, 2)]))
    send_middle(2)
    pass_on(wait1, pass1)
    spread(0, 5, every)
    middle(3, conv(0, [(3, 0), (4, 1), (5, 2)]))
    send_middle(3)
    pass_rest(wait1, pass1)
    for side in range(2):
        pl.when(has_past & from_side[side])(pass1_copy(side).wait_recv)
    receive_edges(PAST)
    for slot in range(2):
        spread(0, slot, every)
    middle(1, conv(0, [(3, 2), (2, 1), (1, 0)]))
    middle(0, conv(0, [(2, 2), (1, 1), (0, 0)]))
    for f in (1, 0):
        send_middle(f)

    for f in (2, 3):
        wait_rows2(f)
    for slot in (4, 5):
        spread(1, slot, outer)
    acc[3] = conv(1, [(4, 1), (5, 2)])
    acc[2] = conv(1, [(4, 2)])
    for f in (1, 0):
        wait_rows2(f)
    for slot in (3, 2):
        spread(1, slot, outer)
    pass_on(wait2[0], pass2[0])
    finish(3, acc[3] + conv(1, [(3, 0)]))
    finish(2, acc[2] + conv(1, [(3, 1), (2, 0)]))
    pass_on(wait2[1], pass2[1])
    acc[1] = conv(1, [(3, 2), (2, 1)])
    acc[0] = conv(1, [(2, 2)])
    for i in range(2):
        pass_rest(wait2[i], pass2[i])
    for i in range(2):
        for side in range(2):
            pl.when(has_past & from_side[side])(pass2_copy(i, side).wait_recv)
    for i in (1, 0):
        spread(1, i, every)
    finish(1, acc[1] + conv(1, [(1, 0)]))
    finish(0, acc[0] + conv(1, [(1, 1), (0, 0)]))

    for dy in (-1, 0, 1):
        for dx in (-1, 1):
            pl.when(at(0, dy, dx)[0])(edge_copy(dy, dx).wait_send)
    for side in range(2):
        @pl.when(to_side[side])
        def _():
            rows1_copy(side).wait_send()
            for f in range(frames):
                rows2_copy(f, side).wait_send()

        @pl.when(to_side[side] & has_past)
        def _():
            pass1_copy(side).wait_send()
            for i in range(2):
                pass2_copy(i, side).wait_send()

    past_edges(has_next, lambda copy: copy.wait_send)

    @pl.when(has_next)
    def _():
        for o in range(rows):
            past1_copy(o).wait_send()
            for i in range(2):
                past2_copy(i, o).wait_send()


def local(features, gain_first, kernel_first, bias_first, gain_second, kernel_second, bias_second):
    frames, rows, cols, ch = features.shape
    lanes = -(-(cols + 4) // 128) * 128
    whole = max(MATMUL, lanes)
    padded = -(-9 * ch // whole) * whole
    per = lanes // (2 * frames * rows)
    blocks = -(-(ch // PACK) // per)
    hbm = pl.BlockSpec(memory_space=pl.ANY)
    bf16, f32 = jnp.bfloat16, jnp.float32
    messages = len(message_numbers(frames, rows))
    dma = pltpu.SemaphoreType.DMA
    result = pl.pallas_call(
        block_kernel,
        out_shape=pltpu.VMEM((frames, rows, ch, cols), bf16),
        in_specs=[hbm] * 7,
        out_specs=pl.BlockSpec(memory_space=pltpu.VMEM),
        scratch_shapes=[
            pltpu.VMEM((frames, rows, ch, cols), bf16),
            pltpu.VMEM((2, 27 * ch, ch), bf16),
            pltpu.VMEM((2, 3, padded // lanes, ch, lanes), bf16),
            pltpu.VMEM((4, 1, ch), f32),
            pltpu.VMEM((4, ch, lanes), f32),
            pltpu.VMEM((2, frames, rows, ch, lanes), bf16),
            pltpu.VMEM((2, 2, rows, ch, lanes), bf16),
            pltpu.VMEM((2, 2, frames + 2, ch, lanes), bf16),
            pltpu.VMEM((2, blocks * PACK, lanes), bf16),
            pltpu.VMEM((2, 3, 2, blocks * PACK, lanes), bf16),
            pltpu.VMEM((2, 3, ch, lanes), bf16),
            pltpu.VMEM((2, frames + 2, 3 * ch, (rows + 2) * lanes), bf16),
            pltpu.VMEM((max(padded - 9 * ch, PACK), rows * lanes), bf16),
            pltpu.VMEM((frames, ch, rows * lanes), f32),
            dma((4,)),
            dma((frames,)),
            dma((2, 3)),
            dma((messages,)),
            dma((messages,)),
        ],
        compiler_params=pltpu.CompilerParams(
            collective_id=0, has_side_effects=True, vmem_limit_bytes=56 * 1024 * 1024
        ),
        name="residual_block",
    )(
        jnp.swapaxes(features, 2, 3),
        gain_first.reshape(1, ch),
        bias_first.reshape(1, ch),
        gain_second.reshape(1, ch),
        bias_second.reshape(1, ch),
        kernel_first.reshape(27 * ch, ch),
        kernel_second.reshape(27 * ch, ch),
    )
    return jnp.swapaxes(result, 2, 3)


def solution(mesh):
    placed = (P("ta", "gy", "gx", None), P(), P(), P(), P(), P(), P())
    return jax.shard_map(
        local, mesh=mesh, in_specs=placed, out_specs=P("ta", "gy", "gx", None), check_vma=False
    )
```

```python
import jax
import jax.numpy as jnp
from jax import lax
from jax.experimental import pallas as pl
from jax.experimental.pallas import tpu as pltpu
from jax.sharding import PartitionSpec as P

epsilon = 1e-06
AXES = ("ta", "gy", "gx")
NOW, PAST = 0, 1
PACK = 16
MATMUL = 256


def activate(field, gain):
    meansq = jnp.mean(field * field, axis=0, keepdims=True)
    u = field * lax.rsqrt(meansq + epsilon) * gain
    half = 0.5 * u
    return half + half * jnp.tanh(half)


def message_numbers(frames, rows):
    names = [("edge", dy, dx) for dy in (-1, 0, 1) for dx in (-1, 1)]
    names += [("past_edge", dy) for dy in (-1, 0, 1)]
    names += [("rows1", side) for side in range(2)]
    names += [("rows2", f, side) for f in range(frames) for side in range(2)]
    names += [("past1", o) for o in range(rows)]
    names += [("past2", i, o) for i in range(2) for o in range(rows)]
    names += [("pass1", side) for side in range(2)]
    names += [("pass2", i, side) for i in range(2) for side in range(2)]
    return {name: n for n, name in enumerate(names)}


def block_kernel(
    feat, gain1, bias1, gain2, bias2, k1, k2, out,
    fin, raw, wt, vec_raw, vec, plane, past, rows_in, edge_out, edge_in, halo, x, zero, acc,
    vec_sem, in_sem, w_sem, send_sem, recv_sem,
):
    frames, rows, ch, cols = fin.shape
    lanes = plane.shape[-1]
    bf16, f32 = jnp.bfloat16, jnp.float32
    taps = 9 * ch
    padded = wt.shape[2] * lanes
    groups = ch // PACK
    width = 2 * frames * rows
    per = lanes // width
    number = message_numbers(frames, rows)
    me = {a: lax.axis_index(a) for a in AXES}
    size = {a: lax.axis_size(a) for a in AXES}
    ta, gy, gx = (me[a] for a in AXES)

    def at(dt, dy, dx):
        place = {"ta": ta + dt, "gy": gy + dy, "gx": gx + dx}
        ok = None
        for a, d in zip(AXES, (dt, dy, dx)):
            if isinstance(d, int) and d == 0:
                continue
            inside = (place[a] >= 0) & (place[a] < size[a])
            ok = inside if ok is None else ok & inside
        return ok, place

    moves = [(0, dy, dx) for dy in (-1, 0, 1) for dx in (-1, 0, 1) if dy or dx]
    moves += [(1, 0, 0)]
    barrier = pltpu.get_barrier_semaphore()
    expected = jnp.int32(0)
    for dt, dy, dx in moves:
        ok, source = at(-dt, -dy, -dx)

        @pl.when(ok)
        def _():
            pl.semaphore_signal(
                barrier, inc=1, device_id=source, device_id_type=pl.DeviceIdType.MESH
            )

        expected = expected + at(dt, dy, dx)[0].astype(jnp.int32)

    fin_copies = [pltpu.make_async_copy(feat.at[f], fin.at[f], in_sem.at[f]) for f in range(frames)]
    for f in reversed(range(frames)):
        fin_copies[f].start()
    vec_copies = [
        pltpu.make_async_copy(v, vec_raw.at[i], vec_sem.at[i])
        for i, v in enumerate((gain1, bias1, gain2, bias2))
    ]
    for copy in vec_copies:
        copy.start()
    w_copies = [
        [
            pltpu.make_async_copy(
                k.at[pl.ds(p * taps, taps)], raw.at[layer, pl.ds(p * taps, taps)], w_sem.at[layer, p]
            )
            for p in range(3)
        ]
        for layer, k in enumerate((k1, k2))
    ]

    def copy_to(name, src, dst, target):
        n = number[name] if isinstance(name, tuple) else name
        return pltpu.make_async_remote_copy(
            src_ref=src,
            dst_ref=dst,
            send_sem=send_sem.at[n],
            recv_sem=recv_sem.at[n],
            device_id=target,
            device_id_type=pl.DeviceIdType.MESH,
        )

    def edge_copy(dy, dx):
        side = (dx + 1) // 2
        target = at(0, dy, dx)[1]
        return copy_to(("edge", dy, dx), edge_out.at[side], edge_in.at[NOW, dy + 1, side], target)

    def past_edge_copy(dy):
        src, dst = edge_in.at[NOW, dy + 1], edge_in.at[PAST, dy + 1]
        return copy_to(("past_edge", dy), src, dst, at(1, 0, 0)[1])

    def past_edges(has, act):
        for dy in (0, -1, 1):
            pl.when(has & from_side[0 if dy > 0 else 1] if dy else has)(act(past_edge_copy(dy)))

    def line(dy):
        return rows - 1 if dy > 0 else 0

    def rows1_copy(side):
        dy = 1 if side == 0 else -1
        src = plane.at[0, :, line(dy)]
        return copy_to(("rows1", side), src, rows_in.at[0, side, pl.ds(2, frames)], at(0, dy, 0)[1])

    def rows2_copy(f, side):
        dy = 1 if side == 0 else -1
        src = plane.at[1, f, line(dy)]
        return copy_to(("rows2", f, side), src, rows_in.at[1, side, 2 + f], at(0, dy, 0)[1])

    def turn(o):
        return jnp.where(gy == 0, rows - 1 - o, o)

    def past1_copy(o):
        r = turn(o)
        src = plane.at[0, pl.ds(frames - 2, 2), r]
        return copy_to(("past1", o), src, past.at[0, :, r], at(1, 0, 0)[1])

    def past2_copy(i, o):
        r = turn(o)
        return copy_to(("past2", i, o), plane.at[1, frames - 2 + i, r], past.at[1, i, r], at(1, 0, 0)[1])

    def pass1_copy(side):
        dy = 1 if side == 0 else -1
        dst = rows_in.at[0, side, pl.ds(0, 2)]
        return copy_to(("pass1", side), past.at[0, :, line(dy)], dst, at(0, dy, 0)[1])

    def pass2_copy(i, side):
        dy = 1 if side == 0 else -1
        dst = rows_in.at[1, side, i]
        return copy_to(("pass2", i, side), past.at[1, i, line(dy)], dst, at(0, dy, 0)[1])

    has_past, has_next = ta > 0, ta < size["ta"] - 1
    from_side = (gy > 0, gy < size["gy"] - 1)
    to_side = (gy < size["gy"] - 1, gy > 0)

    for side in range(2):
        @pl.when(jnp.logical_not(from_side[side]))
        def _():
            rows_in[:, side] = jnp.zeros((2, frames + 2, ch, lanes), bf16)
            edge_in[PAST, 2 - 2 * side] = jnp.zeros(edge_in.shape[2:], bf16)

    @pl.when(jnp.logical_not(has_past))
    def _():
        past[...] = jnp.zeros_like(past)
        rows_in[:, :, 0:2] = jnp.zeros((2, 2, 2, ch, lanes), bf16)
        edge_in[PAST] = jnp.zeros(edge_in.shape[1:], bf16)

    for dy in (-1, 0, 1):
        for dx in (-1, 1):
            @pl.when(jnp.logical_not(at(0, -dy, -dx)[0]))
            def _():
                edge_in[NOW, dy + 1, (dx + 1) // 2] = jnp.zeros(edge_in.shape[3:], bf16)

    plane[0] = jnp.zeros(plane.shape[1:], bf16)
    zero[...] = jnp.zeros_like(zero)
    if padded > taps:
        for layer in range(2):
            for p in range(3):
                for low in range(taps // lanes * lanes, padded, lanes):
                    wt[layer, p, low // lanes] = jnp.zeros((ch, lanes), bf16)
    for i, copy in enumerate(vec_copies):
        copy.wait()
        vec[i] = jnp.broadcast_to(vec_raw[i], (lanes, ch)).T

    lane = lax.broadcasted_iota(jnp.int32, (1, lanes), 1)

    for copy in fin_copies:
        copy.wait()
    for p in (2, 1, 0):
        w_copies[0][p].start()
    for f in reversed(range(frames)):
        for row in range(rows):
            value = activate(fin[f, row].astype(f32), vec[0, :, 0:cols])
            plane[0, f, row, :, 0:cols] = value.astype(bf16)

    def place(v, shift):
        shift = shift % lanes
        return pltpu.roll(v, shift, 1) if shift else v

    lane_pack = lax.broadcasted_iota(jnp.int32, (PACK, lanes), 1)

    def within(low, count):
        return (lane_pack >= low) & (lane_pack < low + count)

    for side in range(2):
        first_col = 0 if side == 0 else cols - 2
        for b in range(edge_out.shape[1] // PACK):
            total = jnp.zeros((PACK, lanes), bf16)
            for f in range(frames):
                for row in range(rows):
                    slot = 2 * (f * rows + row)
                    for g in range(b * per, min(groups, (b + 1) * per)):
                        low = (g - b * per) * width + slot
                        v = plane[0, f, row, g * PACK : (g + 1) * PACK, :]
                        total = jnp.where(within(low, 2), place(v, low - first_col), total)
            edge_out[side, b * PACK : (b + 1) * PACK, :] = total

    pl.semaphore_wait(barrier, expected)
    for dy in (0, -1, 1):
        for dx in (-1, 1):
            pl.when(at(0, dy, dx)[0])(edge_copy(dy, dx).start)
    for side in range(2):
        pl.when(to_side[side])(rows1_copy(side).start)

    @pl.when(has_next)
    def _():
        for o in range(rows):
            past1_copy(o).start()

    for p in (2, 1, 0):
        w_copies[1][p].start()

    def transpose_weights(layer):
        for p in (2, 1, 0):
            w_copies[layer][p].wait()
            for low in range(0, taps, lanes):
                count = min(lanes, taps - low)
                block = raw[layer, p * taps + low : p * taps + low + count, :]
                wt[layer, p, low // lanes, :, 0:count] = block.T

    transpose_weights(0)
    transpose_weights(1)

    def receive_edges(kind):
        if kind == PAST:
            past_edges(has_past, lambda copy: copy.wait_recv)
        else:
            for dy in (-1, 0, 1):
                for dx in (-1, 1):
                    pl.when(at(0, -dy, -dx)[0])(edge_copy(dy, dx).wait_recv)
            past_edges(has_next, lambda copy: copy.start)
        apart = lanes - 2 - cols
        for dy in (-1, 0, 1):
            for g in range(groups):
                b, low = g // per, (g % per) * width
                right = edge_in[kind, dy + 1, 0, b * PACK : (b + 1) * PACK, :]
                left = edge_in[kind, dy + 1, 1, b * PACK : (b + 1) * PACK, :]
                both = jnp.where(within(0, width), place(right, -low), place(left, apart - low))
                halo[kind, dy + 1, g * PACK : (g + 1) * PACK, :] = both

    lane_ch = lax.broadcasted_iota(jnp.int32, (ch, lanes), 1)
    at_halo = ((lane_ch >= cols) & (lane_ch < cols + 2)) | (lane_ch >= lanes - 2)

    def shifts(layer, slot, j, values):
        low, high = j * lanes, (j + len(values)) * lanes
        for r in range(3):
            moved = [place(v, 1 - r) for v in values]
            wide = moved[0] if len(moved) == 1 else jnp.concatenate(moved, axis=1)
            x[layer, slot, r * ch : (r + 1) * ch, low:high] = wide

    def gather(layer, slot, lines):
        values = []
        for j in lines:
            side = 0 if j == 0 else 1
            if j in (0, rows + 1):
                v = rows_in[layer, side, slot]
            elif slot < 2:
                v = past[layer, slot, j - 1]
            else:
                v = plane[layer, slot - 2, j - 1]
            if layer == 0:
                kind = PAST if slot < 2 else NOW
                dy = 1 if j == 0 else -1 if j == rows + 1 else 0
                f = slot + frames - 2 if slot < 2 else slot - 2
                index = 2 * (f * rows + (line(dy) if dy else j - 1))
                v = jnp.where(at_halo, place(halo[kind, dy + 1], cols - index), v)
            values.append(v)
        return values

    def spread(layer, slot, lines):
        if len(lines) == rows + 2 and rows % 2 == 0:
            for j in range(0, rows + 2, 2):
                shifts(layer, slot, j, gather(layer, slot, (j, j + 1)))
        else:
            for j in lines:
                shifts(layer, slot, j, gather(layer, slot, (j,)))

    def conv(layer, terms):
        left, right = [], []
        for slot, p in terms:
            left += [wt[layer, p, c] for c in range(wt.shape[2])]
            for q in range(3):
                right.append(x[layer, slot, :, q * lanes : (q + rows) * lanes])
            if padded > taps:
                right.append(zero[...])
        lhs = jnp.concatenate(left, axis=1)
        rhs = jnp.concatenate(right, axis=0)
        return jnp.dot(lhs, rhs, preferred_element_type=f32)

    keep = (lane < cols) | ((lane == cols) & (gx < size["gx"] - 1)) | ((lane == lanes - 1) & (gx > 0))

    def middle(f, total):
        values = []
        for row in range(rows):
            value = total[:, row * lanes : (row + 1) * lanes] + vec[1]
            value = activate(value.astype(bf16).astype(f32), vec[2])
            value = jnp.where(keep, value, 0.0).astype(bf16)
            plane[1, f, row] = value
            values.append(value)
        held[f] = values

    held = {}

    def send_middle(f):
        for side in range(2):
            pl.when(to_side[side])(rows2_copy(f, side).start)
        if f >= frames - 2:
            @pl.when(has_next)
            def _():
                for o in range(rows):
                    past2_copy(f - frames + 2, o).start()
        shifts(1, f + 2, 1, held[f])

    def finish(f, total):
        for row in range(rows):
            value = total[:, row * lanes : row * lanes + cols] + vec[3, :, 0:cols]
            out[f, row] = (value + fin[f, row].astype(f32)).astype(bf16)

    every = range(rows + 2)
    for side in range(2):
        pl.when(from_side[side])(rows1_copy(side).wait_recv)
    receive_edges(NOW)
    def pass_on(wait, copies):
        @pl.when(has_past)
        def _():
            wait(0)
            for side in range(2):
                for copy in copies(side):
                    pl.when(to_side[side] & (turn(0) == line(1 - 2 * side)))(copy.start)

    def pass_rest(wait, copies):
        @pl.when(has_past)
        def _():
            for o in range(1, rows):
                wait(o)
            for side in range(2) if size["gy"] > 2 else ():
                for copy in copies(side):
                    pl.when(to_side[side] & (turn(0) != line(1 - 2 * side)))(copy.start)

    wait1 = lambda o: past1_copy(o).wait_recv()
    pass1 = lambda side: [pass1_copy(side)]
    wait2 = [lambda o, i=i: past2_copy(i, o).wait_recv() for i in range(2)]
    pass2 = [lambda side, i=i: [pass2_copy(i, side)] for i in range(2)]

    def wait_rows2(f):
        for side in range(2):
            pl.when(from_side[side])(rows2_copy(f, side).wait_recv)

    outer = (0, rows + 1)
    for slot in range(2, 5):
        spread(0, slot, every)
    middle(2, conv(0, [(2, 0), (3, 1), (4, 2)]))
    send_middle(2)
    spread(0, 5, every)
    middle(3, conv(0, [(3, 0), (4, 1), (5, 2)]))
    send_middle(3)
    pass_on(wait1, pass1)
    pass_rest(wait1, pass1)
    for side in range(2):
        pl.when(has_past & from_side[side])(pass1_copy(side).wait_recv)
    receive_edges(PAST)
    for slot in range(2):
        spread(0, slot, every)
    middle(1, conv(0, [(3, 2), (2, 1), (1, 0)]))
    middle(0, conv(0, [(2, 2), (1, 1), (0, 0)]))
    for f in (1, 0):
        send_middle(f)

    for f in (2, 3):
        wait_rows2(f)
    for slot in (4, 5):
        spread(1, slot, outer)
    acc[3] = conv(1, [(4, 1), (5, 2)])
    acc[2] = conv(1, [(4, 2)])
    for f in (1, 0):
        wait_rows2(f)
    for slot in (3, 2):
        spread(1, slot, outer)
    pass_on(wait2[0], pass2[0])
    finish(3, acc[3] + conv(1, [(3, 0)]))
    pass_on(wait2[1], pass2[1])
    finish(2, acc[2] + conv(1, [(3, 1), (2, 0)]))
    acc[1] = conv(1, [(3, 2), (2, 1)])
    acc[0] = conv(1, [(2, 2)])
    for i in range(2):
        pass_rest(wait2[i], pass2[i])
    for i in (1, 0):
        spread(1, i, range(1, rows + 1))
    for dy in (-1, 0, 1):
        for dx in (-1, 1):
            pl.when(at(0, dy, dx)[0])(edge_copy(dy, dx).wait_send)
    for side in range(2):
        @pl.when(to_side[side])
        def _():
            rows1_copy(side).wait_send()
            for f in range(frames):
                rows2_copy(f, side).wait_send()

        pl.when(to_side[side] & has_past)(pass1_copy(side).wait_send)

    past_edges(has_next, lambda copy: copy.wait_send)

    @pl.when(has_next)
    def _():
        for o in range(rows):
            past1_copy(o).wait_send()
            for i in range(2):
                past2_copy(i, o).wait_send()

    for i in range(2):
        for side in range(2):
            pl.when(has_past & from_side[side])(pass2_copy(i, side).wait_recv)
    for i in (1, 0):
        spread(1, i, outer)
    finish(1, acc[1] + conv(1, [(1, 0)]))
    finish(0, acc[0] + conv(1, [(1, 1), (0, 0)]))

    for side in range(2):
        @pl.when(to_side[side] & has_past)
        def _():
            for i in range(2):
                pass2_copy(i, side).wait_send()


def local(features, gain_first, kernel_first, bias_first, gain_second, kernel_second, bias_second):
    frames, rows, cols, ch = features.shape
    lanes = -(-(cols + 4) // 128) * 128
    whole = max(MATMUL, lanes)
    padded = -(-9 * ch // whole) * whole
    per = lanes // (2 * frames * rows)
    blocks = -(-(ch // PACK) // per)
    hbm = pl.BlockSpec(memory_space=pl.ANY)
    bf16, f32 = jnp.bfloat16, jnp.float32
    messages = len(message_numbers(frames, rows))
    dma = pltpu.SemaphoreType.DMA
    result = pl.pallas_call(
        block_kernel,
        out_shape=pltpu.VMEM((frames, rows, ch, cols), bf16),
        in_specs=[hbm] * 7,
        out_specs=pl.BlockSpec(memory_space=pltpu.VMEM),
        scratch_shapes=[
            pltpu.VMEM((frames, rows, ch, cols), bf16),
            pltpu.VMEM((2, 27 * ch, ch), bf16),
            pltpu.VMEM((2, 3, padded // lanes, ch, lanes), bf16),
            pltpu.VMEM((4, 1, ch), f32),
            pltpu.VMEM((4, ch, lanes), f32),
            pltpu.VMEM((2, frames, rows, ch, lanes), bf16),
            pltpu.VMEM((2, 2, rows, ch, lanes), bf16),
            pltpu.VMEM((2, 2, frames + 2, ch, lanes), bf16),
            pltpu.VMEM((2, blocks * PACK, lanes), bf16),
            pltpu.VMEM((2, 3, 2, blocks * PACK, lanes), bf16),
            pltpu.VMEM((2, 3, ch, lanes), bf16),
            pltpu.VMEM((2, frames + 2, 3 * ch, (rows + 2) * lanes), bf16),
            pltpu.VMEM((max(padded - 9 * ch, PACK), rows * lanes), bf16),
            pltpu.VMEM((frames, ch, rows * lanes), f32),
            dma((4,)),
            dma((frames,)),
            dma((2, 3)),
            dma((messages,)),
            dma((messages,)),
        ],
        compiler_params=pltpu.CompilerParams(
            collective_id=0, has_side_effects=True, vmem_limit_bytes=56 * 1024 * 1024
        ),
        name="residual_block",
    )(
        jnp.swapaxes(features, 2, 3),
        gain_first.reshape(1, ch),
        bias_first.reshape(1, ch),
        gain_second.reshape(1, ch),
        bias_second.reshape(1, ch),
        kernel_first.reshape(27 * ch, ch),
        kernel_second.reshape(27 * ch, ch),
    )
    return jnp.swapaxes(result, 2, 3)


def solution(mesh):
    placed = (P("ta", "gy", "gx", None), P(), P(), P(), P(), P(), P())
    return jax.shard_map(
        local, mesh=mesh, in_specs=placed, out_specs=P("ta", "gy", "gx", None), check_vma=False
    )
```
